32 devices in a mesh: dp: 4 (over z), seq: 8 (over y, x, core).
Axes of the slice: x: 2, y: 2, z: 4, core: 2. Of those that a mesh axis runs over, the one named last changes fastest.
Arguments:
- queries: bfloat16 [4, 1024, 2048], P('dp', 'seq'), may hold values from -6 to 6
- keys: bfloat16 [4, 1024, 2048], P('dp', 'seq'), may hold values from -6 to 6
- values: bfloat16 [4, 1024, 2048], P('dp', 'seq'), may hold values from -6 to 6
- residual_in: bfloat16 [4, 1024, 2048], P('dp', 'seq'), may hold values from -6 to 6
- cotangent: bfloat16 [4, 1024, 2048], P('dp', 'seq'), may hold values from -0.09375 to 0.09375
- expert_ids: int32 [4, 1024, 2], P('dp', 'seq'), may hold values from 0 to 7, all different within a row; in each aligned block of 128 rows (0 to 127, 128 to 255, ..., all dimensions but the last counted through in order) at most 48 rows name the same one
- router: bfloat16 [2048, 8], replicated, may hold values from -0.125 to 0.125
- attn_gain: float32 [2048], replicated, may hold values from 0.25 to 1.75
- moe_gain: float32 [2048], replicated, may hold values from 0.25 to 1.75
- w_gate: bfloat16 [8, 2048, 256], P('seq', 'dp'), may hold values from -0.125 to 0.125
- w_up: bfloat16 [8, 2048, 256], P('seq', 'dp'), may hold values from -0.125 to 0.125
- w_down: bfloat16 [8, 2048, 256], P('seq', 'dp'), may hold values from -0.375 to 0.375
- trainable: int32 [8], P('seq'), may hold values 0 or 1
Outputs:
- mixed: bfloat16 [4, 1024, 2048], P('dp', 'seq')
- grad_gate: float32 [8, 2048, 256], P('seq', 'dp')
- grad_up: float32 [8, 2048, 256], P('seq', 'dp')
- grad_down: float32 [8, 2048, 256], P('seq', 'dp')
The draws below stay inside these ranges and needn't reach their ends.
Inputs may be any that keep to these rules, and one draw needn't show every extreme that they name: `expert_ids`: each position names two different experts; among the 128 positions of one index of seq no expert is named by more than 48 choices, a bound that some block reaches.
All inputs are finite; a program needn't handle non-finite values. No bound on the sum of `trainable` on one device may be relied on, other than what follows from the above.
Results may differ from the reference program's by a relative error of at most 0.025.
Values may be sent and summed in bfloat16 or wider, within the bound.
No kernel may reach another device: no remote copies, remote signals or barrier semaphores. Data moves between devices by JAX's collectives and lax.ppermute only.
A program may use at most 128 MiB of HBM per device.

```python
import math
import jax
import jax.numpy as jnp
import numpy as np
from jax import lax

D = 2048
HD = 128
FF = 256
TOK_DEV = 128
HEADS = 16
EXPERTS = 8
CAP = 48
GROUPS = 4
LENGTH = 1024
N_SEQ = 8


def with_ends(array, key, least, largest):
    index_at = [jax.random.randint(jax.random.fold_in(key, axis), (), 0, length) for axis, length in enumerate(array.shape)]
    longest = array.shape.index(max(array.shape))
    beside = index_at[:longest] + [(index_at[longest] + 1) % array.shape[longest]] + index_at[longest + 1:]
    return array.at[tuple(index_at)].set(least).at[tuple(beside)].set(largest)


def shard_levels(key, dims, shards, low, largest):
    def one(position, parts):
        draws = jax.random.uniform(jax.random.fold_in(jax.random.fold_in(key, 6), position), (parts,), jnp.float32, low / len(shards), largest / len(shards))
        return jnp.repeat(jnp.exp(draws), dims[position] // parts).reshape((-1,) + (1,) * (len(dims) - position - 1))

    factor_of = one(*shards[0])
    for cut in shards[1:]:
        factor_of = factor_of * one(*cut)
    return factor_of


def deal_out(rng, own, number, rows, count, top, bound, skew):
    sequence = jax.random.permutation(rng, count)
    heavy_load, common = portions_of(count, rows * top, bound, skew, True), portions_of(count, rows * top, bound, skew, False)
    places = jnp.arange(count)

    def named(lengths, rotation):
        used = int((lengths > 0).sum())
        fixed = max(1, used // 4)
        moved = fixed + (places - fixed + rotation * (used - fixed)) % max(1, count - fixed)
        return jnp.zeros((count,), jnp.int32).at[sequence[jnp.where(places < fixed, places, moved)]].set(jnp.asarray(lengths, jnp.int32))

    lengths = jnp.where(number % 4 == 0, named(heavy_load, number // 4), named(common, number - number // 4 - 1))
    mixed = jax.random.permutation(jax.random.fold_in(own, 3), count)
    donor, receiver = mixed[0:count // 2 * 2:2], mixed[1:count // 2 * 2:2]
    room = jnp.minimum(lengths[donor] - 1, bound - lengths[receiver]) // 2
    room = jnp.where((donor == sequence[0]) | (receiver == sequence[0]) | (lengths[receiver] == 0), 0, jnp.maximum(room, 0))
    moved = jax.random.randint(jax.random.fold_in(own, 4), (count // 2,), 0, 1 << 20) % (room + 1)
    lengths = lengths.at[donor].add(-moved).at[receiver].add(moved)
    items = jnp.searchsorted(jnp.cumsum(lengths), jnp.arange(rows * top), side="right").astype(jnp.int32)
    table = items.reshape(top, rows).T
    table = table[jax.random.permutation(jax.random.fold_in(own, 1), rows)]
    rotation = jax.random.randint(jax.random.fold_in(own, 2), (rows, 1), 0, top)
    return jnp.take_along_axis(table, (jnp.arange(top)[None, :] + rotation) % top, axis=1)


def portions_of(count, total, bound, lean, full):
    loads = [(1 << 20) // math.isqrt(grade ** lean) + 1 for grade in range(1, count + 1)]
    largest = bound if full else min(bound, max(-(-total // count), total * loads[0] // sum(loads)))
    least = 1 if total - largest >= count - 1 else 0
    holding, rest = [largest] + [least] * (count - 1), total - largest - least * (count - 1)
    while rest > 0:
        movable = [i for i in range(1, count) if holding[i] < largest] or [i for i in range(1, count) if holding[i] < bound]
        pool, remaining = sum([loads[i] for i in movable]), rest
        for i in movable:
            more = min(bound - holding[i], max(1, remaining * loads[i] // pool), rest)
            holding[i] = holding[i] + more
            rest = rest - more
    return np.array(holding)


def centred(own_key, dims, spread, reach, pieces=(), kind=jnp.bfloat16):
    result = spread * jax.random.normal(own_key, dims, jnp.float32)
    if pieces:
        result = result * shard_levels(own_key, dims, pieces, -0.22, 0.18)
    return jnp.clip(result, -reach, reach).astype(kind)


def setup_inputs(seed: int = 0) -> dict:
    splits = jax.random.split(jax.random.key(seed), 14)
    queries = centred(splits[0], (GROUPS, LENGTH, D), 1.0, 6.0, ((0, 4), (1, 8)))
    keys = centred(splits[1], (GROUPS, LENGTH, D), 1.0, 6.0, ((0, 4), (1, 8)))
    values = centred(splits[2], (GROUPS, LENGTH, D), 1.0, 6.0, ((0, 4), (1, 8)))
    residual_in = centred(splits[3], (GROUPS, LENGTH, D), 1.0, 6.0, ((0, 4), (1, 8)))
    cotangent = centred(splits[4], (GROUPS, LENGTH, D), 0.015625, 0.09375, ((0, 4), (1, 8)))
    expert_ids_keys = jax.random.split(jax.random.fold_in(splits[5], 1), GROUPS * LENGTH // TOK_DEV)
    expert_ids_turns = jax.random.permutation(jax.random.fold_in(splits[5], 3), GROUPS * LENGTH // TOK_DEV)
    expert_ids = jax.vmap(lambda own, number: deal_out(jax.random.fold_in(splits[5], 2), own, number, TOK_DEV, EXPERTS, 2, CAP, 2))(expert_ids_keys, expert_ids_turns).reshape((GROUPS, LENGTH, 2))
    router = centred(splits[6], (D, EXPERTS), D ** -0.5, 0.125)
    attn_gain = jnp.clip(1.0 + 0.15 * jax.random.normal(splits[7], (D,), jnp.float32), 0.25, 1.75)
    moe_gain = jnp.clip(1.0 + 0.15 * jax.random.normal(splits[8], (D,), jnp.float32), 0.25, 1.75)
    w_gate = centred(splits[9], (EXPERTS, D, FF), D ** -0.5, 0.125, ((0, 8), (1, 4)))
    w_up = centred(splits[10], (EXPERTS, D, FF), D ** -0.5, 0.125, ((0, 8), (1, 4)))
    w_down = centred(splits[11], (EXPERTS, D, FF), FF ** -0.5, 0.375, ((0, 8), (1, 4)))
    trainable = with_ends((jax.random.randint(splits[12], (EXPERTS,), 0, 2) < 1).astype(jnp.int32), jax.random.fold_in(splits[12], 1), 0, 1)
    return {"queries": queries, "keys": keys, "values": values, "residual_in": residual_in, "cotangent": cotangent, "expert_ids": expert_ids, "router": router, "attn_gain": attn_gain, "moe_gain": moe_gain, "w_gate": w_gate, "w_up": w_up, "w_down": w_down, "trainable": trainable}


def to_half(value):
    return lax.optimization_barrier(value.astype(jnp.bfloat16)).astype(jnp.float32)

def attend(queries, keys, values):
    shape = (N_SEQ, TOK_DEV, HEADS, HD)
    qf = queries.astype(jnp.float32).reshape(shape)
    kf = keys.astype(jnp.float32).reshape(shape)
    vf = values.astype(jnp.float32).reshape(shape)
    scores = jnp.einsum('cthd,cshd->chts', qf, kf)
    causal = jnp.tril(jnp.ones((TOK_DEV, TOK_DEV), dtype=bool))
    weights = to_half(jnp.where(causal, scores, 0.0))
    intra = jnp.einsum('chts,cshd->cthd', weights, vf)
    local = jnp.einsum('cthd,cthe->chde', kf, vf)
    prefix = jnp.concatenate([jnp.zeros_like(local[:1]), jnp.cumsum(local[:-1], axis=0)], axis=0)
    carried = jnp.einsum('cthd,chde->cthe', qf, prefix, precision=lax.Precision.HIGHEST)
    attended = intra + carried
    attended = attended * lax.rsqrt(lax.optimization_barrier(jnp.mean(attended * attended, axis=-1, keepdims=True)) + 1e-06)
    return attended.reshape(N_SEQ * TOK_DEV, D)

def one_group(carry, inputs, router, attn_gain, moe_gain, gate32, up32, down32):
    queries, keys, values, residual_in, cotangent, expert_ids = inputs
    length = queries.shape[0]
    stream = residual_in.astype(jnp.float32) + attend(queries, keys, values) * attn_gain
    normed = (stream * lax.rsqrt(lax.optimization_barrier(jnp.mean(stream * stream, axis=-1, keepdims=True)) + 1e-06) * moe_gain).astype(jnp.bfloat16)
    logits = jnp.dot(normed, router, preferred_element_type=jnp.float32)
    onehot = (expert_ids[..., None] == jnp.arange(EXPERTS, dtype=jnp.int32)).astype(jnp.int32)
    chosen = lax.optimization_barrier(jnp.sum(onehot.astype(jnp.float32) * logits[:, None, :], axis=-1))
    sig = jax.nn.sigmoid(chosen)
    gates = sig / lax.optimization_barrier(jnp.sum(sig, axis=-1, keepdims=True))
    flat = onehot.reshape(N_SEQ, 2 * TOK_DEV, EXPERTS)
    before = jnp.cumsum(flat, axis=1) - flat
    rank = lax.optimization_barrier(jnp.sum(before * flat, axis=-1)).astype(jnp.int32)
    chosen_ids = expert_ids.reshape(N_SEQ, 2 * TOK_DEV).astype(jnp.int32)
    rows = N_SEQ * CAP
    dest = (chosen_ids * rows + jnp.arange(N_SEQ, dtype=jnp.int32)[:, None] * CAP + rank).reshape(-1)
    repeated = jnp.repeat(normed, 2, axis=0)
    bucket = jnp.zeros((EXPERTS * rows, D), jnp.bfloat16).at[dest].set(repeated)
    expert_cot = (cotangent.astype(jnp.float32)[:, None, :] * gates[:, :, None]).reshape(2 * length, D).astype(jnp.bfloat16)
    cot_bucket = jnp.zeros((EXPERTS * rows, D), jnp.bfloat16).at[dest].set(expert_cot)
    xf = lax.optimization_barrier(bucket).astype(jnp.float32).reshape(EXPERTS, rows, D)
    dyf = lax.optimization_barrier(cot_bucket).astype(jnp.float32).reshape(EXPERTS, rows, D)
    pre_gate = jnp.einsum('erd,edf->erf', xf, gate32)
    pre_up = jnp.einsum('erd,edf->erf', xf, up32)
    sigma = jax.nn.sigmoid(pre_gate)
    act = pre_gate * sigma
    hidden = to_half(act * pre_up)
    expert_out = jnp.einsum('erf,edf->erd', hidden, down32).astype(jnp.bfloat16)
    gathered = expert_out.reshape(EXPERTS * rows, D)[dest].astype(jnp.float32).reshape(length, 2, D)
    mixed = (stream + lax.optimization_barrier(jnp.sum(gates[:, :, None] * gathered, axis=1))).astype(jnp.bfloat16)
    d_hidden = jnp.einsum('erd,edf->erf', dyf, down32)
    d_gate = to_half(d_hidden * pre_up * sigma * (1.0 + pre_gate * (1.0 - sigma)))
    d_up = to_half(d_hidden * act)
    part_gate = to_half(jnp.einsum('erd,erf->edf', xf, d_gate))
    part_up = to_half(jnp.einsum('erd,erf->edf', xf, d_up))
    part_down = to_half(jnp.einsum('erd,erf->edf', dyf, hidden))
    carry = (carry[0] + part_gate, carry[1] + part_up, carry[2] + part_down)
    return (carry, mixed)

def reference(queries, keys, values, residual_in, cotangent, expert_ids, router, attn_gain, moe_gain, w_gate, w_up, w_down, trainable):
    gate32 = w_gate.astype(jnp.float32)
    up32 = w_up.astype(jnp.float32)
    down32 = w_down.astype(jnp.float32)
    zeros = jnp.zeros((EXPERTS, D, FF), jnp.float32)

    def step(carry, inputs):
        return one_group(carry, inputs, router, attn_gain, moe_gain, gate32, up32, down32)
    totals, mixed = lax.scan(step, (zeros, zeros, zeros), (queries, keys, values, residual_in, cotangent, expert_ids))
    flag = (trainable > 0).astype(jnp.float32)[:, None, None]
    return (mixed, totals[0] * flag, totals[1] * flag, totals[2] * flag)
```

```python
import jax
import jax.numpy as jnp
from jax import lax
from jax.sharding import PartitionSpec as P

HD = 128
F32 = jnp.float32
BF16 = jnp.bfloat16
ROWS = (((0,), (0,)), ((), ()))


def exclusive_prefix(local, axis):
    n, i = lax.axis_size(axis), lax.axis_index(axis)
    half = local.shape[0] // 2
    core = i % 2
    mine = lax.dynamic_slice_in_dim(local, core * half, half, 0)
    other = lax.dynamic_slice_in_dim(local, (1 - core) * half, half, 0)
    swap = [(j, j ^ 1) for j in range(n)]
    peer = lax.ppermute(other, axis, swap).astype(F32)
    mine = mine.astype(F32)
    total = mine + peer
    before = jnp.zeros_like(total)
    step = 2
    while step < n:
        last = 2 * step >= n
        pairs = [(j, j ^ step) for j in range(n) if not (last and j & step)]
        got = lax.ppermute(total.astype(BF16), axis, pairs).astype(F32)
        before = before + jnp.where((i & step) != 0, got, 0.0)
        total = total + got
        step *= 2
    own = before + jnp.where(core == 1, peer, 0.0)
    theirs = before + jnp.where(core == 0, mine, 0.0)
    back = lax.ppermute(theirs.astype(BF16), axis, swap)
    own = own.astype(BF16)
    return jnp.where(core == 0, jnp.concatenate([own, back], 0), jnp.concatenate([back, own], 0))


def gather_line(x, axis):
    n = lax.axis_size(axis)
    right, left = [x], [x]
    for k in range(1, n):
        right.append(lax.ppermute(right[-1], axis, [(j, j + 1) for j in range(k - 1, n - 1)]))
        left.append(lax.ppermute(left[-1], axis, [(j, j - 1) for j in range(1, n - k + 1)]))
    return [x] + [left[d] + right[n - d] for d in range(1, n)]


def scatter_line(parts, axis):
    n, i = lax.axis_size(axis), lax.axis_index(axis)
    right = left = None
    for k in range(n - 1, 0, -1):
        send_r, send_l = parts[k], parts[n - k]
        if right is not None:
            send_r = (send_r.astype(F32) + right.astype(F32)).astype(BF16)
            send_l = (send_l.astype(F32) + left.astype(F32)).astype(BF16)
        right = lax.ppermute(send_r, axis, [(j, j + 1) for j in range(0, n - k)])
        left = lax.ppermute(send_l, axis, [(j, j - 1) for j in range(k, n)])
    return parts[0].astype(F32) + right.astype(F32) + left.astype(F32)


def exchange(x):
    return lax.all_to_all(x, "seq", split_axis=0, concat_axis=0, tiled=True)


def body(
    queries,
    keys,
    values,
    residual_in,
    cotangent,
    expert_ids,
    router,
    attn_gain,
    moe_gain,
    w_gate,
    w_up,
    w_down,
    trainable,
):
    tokens = queries.shape[1]
    width = queries.shape[2]
    heads = width // HD
    experts = router.shape[1]
    peers = lax.axis_size("seq")
    groups = lax.axis_size("dp")
    slots = max(2, 3 * tokens // peers)
    part = width // groups
    ff = w_gate.shape[2]
    shift = lax.axis_index("dp") * part
    me = lax.axis_index("seq")

    weights = gather_line(jnp.concatenate([w_gate[0], w_up[0], w_down[0]], axis=1), "dp")

    q_heads = queries[0].reshape(tokens, heads, HD)
    k_heads = keys[0].reshape(tokens, heads, HD)
    v_heads = values[0].reshape(tokens, heads, HD)
    local = jnp.einsum("thd,the->hde", k_heads, v_heads, preferred_element_type=F32).astype(BF16)
    prefix = exclusive_prefix(local, "seq")

    choices_ids = expert_ids[0]
    onehot = (choices_ids[..., None] == jnp.arange(experts, dtype=jnp.int32)).astype(jnp.int32)
    flat = onehot.reshape(2 * tokens, experts)
    before = jnp.cumsum(flat, axis=0) - flat
    rank = jnp.sum(before * flat, axis=-1)
    target = (choices_ids.reshape(2 * tokens) * slots + rank).reshape(tokens, 2)
    places = jnp.arange(experts * slots, dtype=jnp.int32)[None, :]
    first = target[:, 0:1] == places
    second = target[:, 1:2] == places
    both = (first | second).astype(BF16)
    pick_0, pick_1 = first.astype(BF16), second.astype(BF16)
    others = choices_ids.astype(BF16)
    spread = lambda column: jnp.broadcast_to(column, (tokens, HD))
    other_rows = lax.dot_general(
        pick_0, spread(others[:, 1:2]), ROWS, preferred_element_type=F32
    ) + lax.dot_general(pick_1, spread(others[:, 0:1]), ROWS, preferred_element_type=F32)

    rolled_cot = jnp.roll(cotangent[0], -shift, axis=1)
    cot_send = jnp.concatenate(
        [
            lax.dot_general(both, rolled_cot, ROWS, preferred_element_type=F32).astype(BF16),
            other_rows.astype(BF16),
        ],
        axis=1,
    )
    cot_got = exchange(cot_send.reshape(experts, slots, width + HD)).reshape(
        peers * slots, width + HD
    )
    cot_rows = cot_got[:, :width]
    other_id = cot_got[:, width : width + 1].astype(F32)

    scores = jnp.einsum("thd,shd->hts", q_heads, k_heads, preferred_element_type=F32)
    causal = jnp.tril(jnp.ones((tokens, tokens), dtype=bool))
    mask_scores = jnp.where(causal, scores, 0.0).astype(BF16)
    intra = jnp.einsum("hts,shd->thd", mask_scores, v_heads, preferred_element_type=F32)
    carried = jnp.einsum("thd,hde->the", q_heads, prefix, preferred_element_type=F32)
    attended = intra + carried
    attended = attended * lax.rsqrt(jnp.mean(attended * attended, axis=-1, keepdims=True) + 1e-06)
    stream = residual_in[0].astype(F32) + attended.reshape(tokens, width) * attn_gain
    normed = (
        stream * lax.rsqrt(jnp.mean(stream * stream, axis=-1, keepdims=True) + 1e-06) * moe_gain
    ).astype(BF16)
    rolled = jnp.roll(normed, -shift, axis=1)
    send_rows = lax.dot_general(both, rolled, ROWS, preferred_element_type=F32).astype(BF16)
    rows = exchange(send_rows.reshape(experts, slots, width)).reshape(peers * slots, width)

    logits = jnp.dot(normed, router, preferred_element_type=F32)
    chosen = jnp.sum(onehot.astype(F32) * logits[:, None, :], axis=-1)
    sig = jax.nn.sigmoid(chosen)
    gates = sig / jnp.sum(sig, axis=-1, keepdims=True)

    row_logits = jnp.dot(rows, jnp.roll(router, -shift, axis=0), preferred_element_type=F32)
    lanes = jnp.arange(experts, dtype=jnp.int32)[None, :]
    row_sig = jax.nn.sigmoid(row_logits)
    own_sig = jnp.sum(jnp.where(lanes == me, row_sig, 0.0), axis=1, keepdims=True)
    other_sig = jnp.sum(
        jnp.where(lanes == other_id.astype(jnp.int32), row_sig, 0.0), axis=1, keepdims=True
    )
    row_gate = own_sig / (own_sig + other_sig)

    pre = d_hidden = 0.0
    for d in range(groups):
        block = slice(d * part, (d + 1) * part)
        pre = pre + jnp.dot(
            rows[:, block], weights[d][:, : 2 * ff], preferred_element_type=F32
        )
        d_hidden = d_hidden + jnp.dot(
            cot_rows[:, block], weights[d][:, 2 * ff :], preferred_element_type=F32
        )
    d_hidden = d_hidden * row_gate
    pre_gate, pre_up = pre[:, :ff], pre[:, ff:]
    sigma = jax.nn.sigmoid(pre_gate)
    act = pre_gate * sigma
    hidden_wide = act * pre_up
    hidden = hidden_wide.astype(BF16)
    gated = (hidden_wide * row_gate).astype(BF16)
    d_gate = d_hidden * pre_up * sigma * (1.0 + pre_gate * (1.0 - sigma))
    d_up = d_hidden * act
    d_both = jnp.concatenate([d_gate, d_up], axis=1).astype(BF16)

    expert_out = jnp.concatenate(
        [
            lax.dot_general(
                hidden, weights[d][:, 2 * ff :], (((1,), (1,)), ((), ())), preferred_element_type=F32
            ).astype(BF16)
            for d in range(groups)
        ],
        axis=1,
    )
    back = exchange(expert_out.reshape(peers, slots, width)).reshape(experts * slots, width)

    terms = []
    for d in range(groups):
        block = slice(d * part, (d + 1) * part)
        both_terms = lax.dot_general(rows[:, block], d_both, ROWS, preferred_element_type=F32)
        down_term = lax.dot_general(cot_rows[:, block], gated, ROWS, preferred_element_type=F32)
        terms.append(jnp.concatenate([both_terms, down_term], axis=1).astype(BF16))
    scale = (trainable[0] > 0).astype(F32)
    summed = scatter_line(terms, "dp") * scale

    weight = (
        jnp.where(first, gates[:, 0:1], 0.0) + jnp.where(second, gates[:, 1:2], 0.0)
    ).astype(BF16)
    expert_part = jnp.roll(jnp.dot(weight, back, preferred_element_type=F32), shift, axis=1)
    mixed = (stream + expert_part).astype(BF16)
    return (
        mixed[None],
        summed[None, :, :ff],
        summed[None, :, ff : 2 * ff],
        summed[None, :, 2 * ff :],
    )


def solution(mesh):
    return jax.shard_map(
        body,
        mesh=mesh,
        in_specs=(
            P("dp", "seq", None),
            P("dp", "seq", None),
            P("dp", "seq", None),
            P("dp", "seq", None),
            P("dp", "seq", None),
            P("dp", "seq", None),
            P(),
            P(),
            P(),
            P("seq", "dp", None),
            P("seq", "dp", None),
            P("seq", "dp", None),
            P("seq"),
        ),
        out_specs=(
            P("dp", "seq", None),
            P("seq", "dp", None),
            P("seq", "dp", None),
            P("seq", "dp", None),
        ),
        check_vma=False,
    )
```

```python
import functools

import jax
import jax.numpy as jnp
from jax import lax
from jax.experimental import pallas as pl
from jax.experimental.pallas import tpu as pltpu
from jax.sharding import PartitionSpec as P


HD = 128
F32 = jnp.float32
BF16 = jnp.bfloat16
MATMUL = (((1,), (0,)), ((), ()))
ROWS = (((0,), (0,)), ((), ()))
LANES = (((1,), (1,)), ((), ()))


def dot(a, b, dims=MATMUL):
    return lax.dot_general(a, b, dims, preferred_element_type=F32)


def kernel_call(body, ins, outs, scratch=(), flops=1_000_000_000, **static):
    place = {"s": pltpu.SMEM, "v": pltpu.VMEM, "h": pltpu.HBM}

    def call(*operands):
        letters = ins + ins[-1] * (len(operands) - len(ins))
        operands = [
            pltpu.with_memory_space_constraint(y, pltpu.HBM) if x == "h" else y
            for x, y in zip(letters, operands)
        ]
        return pl.pallas_call(
            functools.partial(body, **static),
            in_specs=[pl.BlockSpec(memory_space=place[x]) for x in letters],
            out_specs=[pl.BlockSpec(memory_space=place[x]) for x, _, _ in outs],
            out_shape=[
                (pltpu.HBM if x == "h" else jax.ShapeDtypeStruct)(shape, kind)
                for x, shape, kind in outs
            ],
            scratch_shapes=list(scratch),
            cost_estimate=pl.CostEstimate(flops=flops, bytes_accessed=4_000_000, transcendentals=0),
            compiler_params=pltpu.CompilerParams(vmem_limit_bytes=48 * 1024 * 1024),
        )(*operands)

    return call


class Copies:
    def __init__(self, sems):
        self.sems, self.n = sems, 0

    def start(self, source, target):
        copy = pltpu.make_async_copy(source, target, self.sems.at[self.n])
        self.n += 1
        copy.start()
        return copy


def route_kernel(
    i_ref, me_ref, ids_ref, cot_hbm, put_ref, slot_ref, *refs, groups, slots
):
    sends, (cot_ref, buf, sems) = refs[:-3], refs[-3:]
    tokens, rows_n = put_ref.shape
    width = cot_ref.shape[1]
    part = width // groups
    copies = Copies(sems)
    loads = []
    for d in range(groups):
        source = pl.multiple_of((i_ref[0] ^ d) * part, HD)
        loads.append(
            copies.start(
                cot_hbm.at[0, :, pl.ds(source, part)], cot_ref.at[:, pl.ds(d * part, part)]
            )
        )
    id_0, id_1 = ids_ref[0, :, 0:1], ids_ref[0, :, 1:2]
    lanes = lax.broadcasted_iota(jnp.int32, (tokens, HD), 1)
    hit_0, hit_1 = lanes == id_0, lanes == id_1
    count = jnp.where(hit_0, 1.0, jnp.where(hit_1, 1.0, 0.0)).astype(BF16)
    row = lax.broadcasted_iota(jnp.int32, (tokens, tokens), 0)
    col = lax.broadcasted_iota(jnp.int32, (tokens, tokens), 1)
    before = dot(jnp.where(row > col, 1.0, 0.0).astype(BF16), count)
    rank_0 = jnp.sum(jnp.where(hit_0, before, 0.0), axis=1, keepdims=True).astype(jnp.int32)
    rank_1 = jnp.sum(jnp.where(hit_1, before, 0.0), axis=1, keepdims=True).astype(jnp.int32)
    slot_0, slot_1 = id_0 * slots + rank_0, id_1 * slots + rank_1
    slot_ref[:, 0:1] = slot_0
    slot_ref[:, 1:2] = slot_1
    wide = lax.broadcasted_iota(jnp.int32, (tokens, rows_n), 1)
    put = jnp.where(wide == slot_0, 1.0, jnp.where(wide == slot_1, 1.0, 0.0)).astype(BF16)
    put_ref[...] = put
    both = jnp.broadcast_to((id_0 + id_1).astype(F32), (tokens, HD)).astype(BF16)
    buf[:, pl.ds(width, HD)] = dot(put, both, ROWS).astype(BF16)
    for d in range(groups):
        at = pl.ds(d * part, part)
        loads[d].wait()
        buf[:, at] = dot(put, cot_ref[:, at], ROWS).astype(BF16)
    if len(sends) == 1:
        stores = [copies.start(buf, sends[0])]
    else:
        stores = [
            copies.start(buf.at[pl.ds(pl.multiple_of((me_ref[0] ^ k) * slots, 16), slots)], send)
            for k, send in enumerate(sends)
        ]
    for copy in stores:
        copy.wait()


def load_rows(copies, me, pieces, target, slots):
    if len(pieces) == 1:
        return [copies.start(pieces[0], target)]
    return [
        copies.start(piece, target.at[pl.ds(pl.multiple_of((me ^ k) * slots, 16), slots)])
        for k, piece in enumerate(pieces)
    ]


def state_kernel(k_hbm, v_hbm, out_ref, k_ref, v_ref, sems, *, heads, chunks):
    copies = Copies(sems)
    size = heads // chunks
    loads = []
    for c in range(chunks):
        at = pl.ds(c * size * HD, size * HD)
        loads.append(
            [
                copies.start(k_hbm.at[0, :, at], k_ref.at[:, at]),
                copies.start(v_hbm.at[0, :, at], v_ref.at[:, at]),
            ]
        )
    for h in range(heads):
        if h % size == 0:
            for copy in loads[h // size]:
                copy.wait()
        at = pl.ds(h * HD, HD)
        out_ref[h] = dot(k_ref[:, at], v_ref[:, at], ROWS).astype(BF16)


def intra_kernel(q_ref, k_ref, v_ref, out_ref, *, heads):
    tokens = q_ref.shape[1]
    row = lax.broadcasted_iota(jnp.int32, (tokens, tokens), 0)
    col = lax.broadcasted_iota(jnp.int32, (tokens, tokens), 1)
    causal = row >= col
    for h in range(heads):
        at = pl.ds(h * HD, HD)
        scores = dot(q_ref[0, :, at], k_ref[0, :, at], LANES)
        scores = jnp.where(causal, scores, 0.0).astype(BF16)
        out_ref[:, at] = dot(scores, v_ref[0, :, at])


def norm_kernel(
    i_ref, q_ref, prefix_ref, intra_ref, residual_ref, attn_ref, moe_ref, put_ref,
    stream_out, normed_out, send_out, stream_ref, normed_ref, send_ref, sems, *, heads, groups,
):
    tokens, width = stream_ref.shape
    copies, started = Copies(sems), []
    squares = jnp.zeros((tokens, HD), F32)
    for h in range(heads):
        at = pl.ds(h * HD, HD)
        attended = intra_ref[:, at] + dot(q_ref[0, :, at], prefix_ref[h])
        mean = jnp.mean(attended * attended, axis=-1, keepdims=True)
        attended = attended * lax.rsqrt(mean + 1e-06)
        stream = residual_ref[0, :, at].astype(F32) + attended * attn_ref[:, at]
        stream_ref[:, at] = stream
        squares = squares + stream * stream
    scale = lax.rsqrt(jnp.sum(squares, axis=-1, keepdims=True) / width + 1e-06)
    part = width // groups
    for h in range(heads):
        at = pl.ds(h * HD, HD)
        normed_ref[:, at] = (stream_ref[:, at] * scale * moe_ref[:, at]).astype(BF16)
    put = put_ref[...]
    for d in range(groups):
        at = pl.ds(d * part, part)
        source = pl.multiple_of((i_ref[0] ^ d) * part, HD)
        send_ref[:, at] = dot(put, normed_ref[:, pl.ds(source, part)], ROWS).astype(BF16)
        started.append(copies.start(send_ref.at[:, at], send_out.at[:, at]))
    started.append(copies.start(normed_ref, normed_out))
    started.append(copies.start(stream_ref, stream_out))
    for copy in started:
        copy.wait()


def expert_kernel(me_ref, router_ref, rows_hbm, *refs, groups, gathered, pieces, slots):
    own, got, cots = refs[:3], refs[3 : 3 + gathered], refs[3 + gathered : 3 + gathered + pieces]
    hidden_ref, gated_ref, delta_ref, term_ref = refs[3 + gathered + pieces : -4]
    rows_ref, cot_ref, w_ref, sems = refs[-4:]
    rows_n, width = rows_ref.shape
    part = width // groups
    ff = hidden_ref.shape[1]
    copies = Copies(sems)
    loads = []
    for d in range(groups):
        at = pl.ds(d * part, part)
        load = [copies.start(rows_hbm.at[:, at], rows_ref.at[:, at])]
        if d == 0:
            for n in range(3):
                load.append(copies.start(own[n].at[0], w_ref.at[0, :, pl.ds(n * ff, ff)]))
        else:
            load.append(copies.start(got[d - 1], w_ref.at[d]))
            if d == groups - 1 and gathered == groups:
                load.append(copies.start(got[d], w_ref.at[d + 1]))
        loads.append(load)
    cot_loads = load_rows(copies, me_ref[0], cots, cot_ref, slots)
    cuts = [pl.ds(n * ff, ff) for n in range(3)]
    pre_gate, pre_up, d_hidden = (jnp.zeros((rows_n, ff), F32) for _ in range(3))
    logits = jnp.zeros((rows_n, router_ref.shape[0]), F32)
    for d in range(groups):
        at = pl.ds(d * part, part)
        for copy in loads[d]:
            copy.wait()
        if d == groups - 1 and gathered == groups:
            w_ref[d] = w_ref[d] + w_ref[d + 1]
        block = rows_ref[:, at]
        pre_gate = pre_gate + dot(block, w_ref[d, :, cuts[0]])
        pre_up = pre_up + dot(block, w_ref[d, :, cuts[1]])
        logits = logits + dot(block, router_ref[:, at], LANES)
    for copy in cot_loads:
        copy.wait()
    for d in range(groups):
        d_hidden = d_hidden + dot(cot_ref[:, pl.ds(d * part, part)], w_ref[d, :, cuts[2]])
    lanes = lax.broadcasted_iota(jnp.int32, logits.shape, 1)
    me = me_ref[0]
    other = cot_ref[:, pl.ds(width, HD)].astype(F32).astype(jnp.int32)[:, : logits.shape[1]] - me
    sig = 1.0 / (1.0 + jnp.exp(-logits))
    own_sig = jnp.sum(jnp.where(lanes == me, sig, 0.0), axis=1, keepdims=True)
    other_sig = jnp.sum(jnp.where(lanes == other, sig, 0.0), axis=1, keepdims=True)
    gate = own_sig / (own_sig + other_sig)
    d_hidden = d_hidden * gate
    sigma = 1.0 / (1.0 + jnp.exp(-pre_gate))
    act = pre_gate * sigma
    hidden = act * pre_up
    hidden_ref[...] = hidden.astype(BF16)
    gated_ref[...] = (hidden * gate).astype(BF16)
    delta_ref[:, :ff] = (d_hidden * pre_up * sigma * (1.0 + pre_gate * (1.0 - sigma))).astype(BF16)
    delta_ref[:, ff:] = (d_hidden * act).astype(BF16)
    term(rows_ref, cot_ref, delta_ref, gated_ref, term_ref, (groups - 1) * part)


def term(rows_ref, cot_ref, delta_ref, gated_ref, out_ref, start):
    part = out_ref.shape[0]
    ff = gated_ref.shape[1]
    at = pl.ds(start, part)
    out_ref[:, : 2 * ff] = dot(rows_ref[:, at], delta_ref[...], ROWS).astype(BF16)
    out_ref[:, 2 * ff :] = dot(cot_ref[:, at], gated_ref[...], ROWS).astype(BF16)


def output_kernel(
    me_ref, hidden_ref, gated_ref, delta_ref, rows_hbm, *refs, groups, gathered, pieces, slots
):
    own, got, cots = refs[:1], refs[1 : 1 + gathered], refs[1 + gathered : 1 + gathered + pieces]
    out_hbm, near_hbm, *terms = refs[1 + gathered + pieces : -6]
    rows_ref, cot_ref, w_ref, out_ref, near_ref, sems = refs[-6:]
    _, width = rows_ref.shape
    part = width // groups
    ff = hidden_ref.shape[1]
    copies = Copies(sems)
    row_load = copies.start(rows_hbm, rows_ref)
    cot_loads = load_rows(copies, me_ref[0], cots, cot_ref, slots)
    loads = [[copies.start(own[0].at[0], w_ref.at[0])]]
    for d in range(1, groups):
        at = pl.ds(2 * ff, ff)
        load = [copies.start(got[d - 1].at[:, at], w_ref.at[d])]
        if d == groups - 1 and gathered == groups:
            load.append(copies.start(got[d].at[:, at], w_ref.at[d + 1]))
        loads.append(load)
    row_load.wait()
    for copy in cot_loads:
        copy.wait()
    term(rows_ref, cot_ref, delta_ref, gated_ref, near_ref, part)
    stores = [copies.start(near_ref, near_hbm)]
    for n, out in enumerate(terms):
        term(rows_ref, cot_ref, delta_ref, gated_ref, out, (0 if n == 0 else n + 1) * part)
    for d in range(groups):
        for copy in loads[d]:
            copy.wait()
        if d == groups - 1 and gathered == groups:
            w_ref[d] = w_ref[d] + w_ref[d + 1]
        at = pl.ds(d * part, part)
        out_ref[:, at] = dot(hidden_ref[...], w_ref[d], LANES).astype(BF16)
        stores.append(copies.start(out_ref.at[:, at], out_hbm.at[:, at]))
    for copy in stores:
        copy.wait()


def combine_kernel(
    i_ref, stream_ref, normed_ref, router_ref, ids_ref, slot_ref, back_ref, out_ref, *, groups
):
    tokens, width = stream_ref.shape
    rows_n = back_ref.shape[0]
    logits = dot(normed_ref[...], router_ref[...], LANES)
    sig = 1.0 / (1.0 + jnp.exp(-logits))
    lanes = lax.broadcasted_iota(jnp.int32, logits.shape, 1)
    sig_0, sig_1 = (
        jnp.sum(jnp.where(lanes == ids_ref[0, :, j : j + 1], sig, 0.0), axis=1, keepdims=True)
        for j in range(2)
    )
    total = sig_0 + sig_1
    wide = lax.broadcasted_iota(jnp.int32, (tokens, rows_n), 1)
    take = jnp.where(
        wide == slot_ref[:, 0:1],
        sig_0 / total,
        jnp.where(wide == slot_ref[:, 1:2], sig_1 / total, 0.0),
    ).astype(BF16)
    part = width // groups
    for d in range(groups):
        at = pl.ds(pl.multiple_of((i_ref[0] ^ d) * part, HD), part)
        value = stream_ref[:, at] + dot(take, back_ref[:, pl.ds(d * part, part)])
        out_ref[0, :, at] = value.astype(BF16)


def total_kernel(scale_ref, *refs):
    parts, outs = refs[:-3], refs[-3:]
    ff = outs[0].shape[1]
    scale = jnp.where(scale_ref[0] > 0, 1.0, 0.0)
    for n, out in enumerate(outs):
        at = pl.ds(n * ff, ff)
        value = parts[0][:, at].astype(F32)
        for other in parts[1:]:
            value = value + other[:, at].astype(F32)
        out[...] = value * scale


def exclusive_prefix(local, axis):
    n, i = lax.axis_size(axis), lax.axis_index(axis)
    half = local.shape[0] // 2
    core = i % 2
    mine = lax.dynamic_slice_in_dim(local, core * half, half, 0)
    other = lax.dynamic_slice_in_dim(local, (1 - core) * half, half, 0)
    swap = [(j, j ^ 1) for j in range(n)]
    peer = lax.ppermute(other, axis, swap).astype(F32)
    mine = mine.astype(F32)
    total = (mine + peer).astype(BF16)
    before = jnp.zeros_like(mine)
    far = [lax.ppermute(total, axis, [(j, j + d) for j in range(n - d)]) for d in range(2, n, 2)]
    for got in far:
        before = before + got.astype(F32)
    own = before + jnp.where(core == 1, peer, 0.0)
    theirs = before + jnp.where(core == 0, mine, 0.0)
    back = lax.ppermute(theirs.astype(BF16), axis, swap)
    own = own.astype(BF16)
    return jnp.where(core == 0, jnp.concatenate([own, back], 0), jnp.concatenate([back, own], 0))


def send_xor(x, axis, d):
    return lax.ppermute(x, axis, [(j, j ^ d) for j in range(lax.axis_size(axis))])


ENDS = [(0, 1), (3, 2)]
MIDDLE = [(1, 2), (2, 1)]


def gather_xor(x, axis):
    n = lax.axis_size(axis)
    if n != 4:
        return [send_xor(x, axis, d) for d in range(1, n)]
    near, across = send_xor(x, axis, 1), send_xor(x, axis, 2)
    relayed = lax.ppermute(across, axis, [(b, a) for a, b in ENDS])
    middle = lax.ppermute(x, axis, MIDDLE)
    return [near, across, relayed, middle]


def scatter_xor(parts, axis):
    n = lax.axis_size(axis)
    if n != 4:
        return [parts[0]] + [send_xor(parts[d], axis, d) for d in range(1, n)]
    relayed = lax.ppermute(parts[3], axis, ENDS)
    middle = lax.ppermute(parts[3], axis, MIDDLE)
    merged = (parts[2].astype(F32) + relayed.astype(F32)).astype(BF16)
    across = send_xor(merged, axis, 2)
    near = send_xor(parts[1], axis, 1)
    return [parts[0], middle, across, near]


def exchange(x):
    return lax.all_to_all(x, "seq", split_axis=0, concat_axis=0, tiled=True)


def exchange_pieces(blocks):
    return [blocks[0]] + [
        send_xor(blocks[k], "seq", k) for k in range(len(blocks) - 1, 0, -1)
    ][::-1]


def swap_blocks(x, axis, dim):
    n, i = lax.axis_size(axis), lax.axis_index(axis)
    size = x.shape[dim] // n
    return jnp.concatenate(
        [lax.dynamic_slice_in_dim(x, (i ^ d) * size, size, dim) for d in range(n)], axis=dim
    )


def layer(
    queries,
    keys,
    values,
    residual_in,
    cotangent,
    expert_ids,
    router,
    attn_gain,
    moe_gain,
    w_gate,
    w_up,
    w_down,
    trainable,
):
    tokens = queries.shape[1]
    width = queries.shape[2]
    heads = width // HD
    experts = router.shape[1]
    peers = lax.axis_size("seq")
    groups = lax.axis_size("dp")
    slots = max(2, 3 * tokens // peers)
    rows_n = experts * slots
    part = width // groups
    ff = w_gate.shape[2]
    i = lax.axis_index("dp")[None]
    me = lax.axis_index("seq")[None]
    turned = swap_blocks(router.T, "dp", 1)

    split = slots % 16 == 0
    cot_shape = (slots if split else rows_n, width + HD)
    pieces = peers if split else 1
    put, slot, *cot_send = kernel_call(
        route_kernel,
        "ssvh",
        [("v", (tokens, rows_n), BF16), ("v", (tokens, 2), jnp.int32)]
        + [("h", cot_shape, BF16)] * pieces,
        [
            pltpu.VMEM((tokens, width), BF16),
            pltpu.VMEM((rows_n, width + HD), BF16),
            pltpu.SemaphoreType.DMA((groups + pieces,)),
        ],
        groups=groups,
        slots=slots,
    )(i, me, expert_ids, cotangent)
    if split:
        cots = exchange_pieces(cot_send)
    else:
        cots = [exchange(cot_send[0].reshape(experts, slots, -1)).reshape(cot_shape)]

    got = gather_xor(jnp.concatenate([w_gate[0], w_up[0], w_down[0]], axis=1), "dp")
    own = [w_gate, w_up, w_down]

    (local,) = kernel_call(
        state_kernel,
        "h",
        [("v", (heads, HD, HD), BF16)],
        [
            pltpu.VMEM((tokens, width), BF16),
            pltpu.VMEM((tokens, width), BF16),
            pltpu.SemaphoreType.DMA((8,)),
        ],
        heads=heads,
        chunks=4,
    )(keys, values)
    prefix = exclusive_prefix(local, "seq")

    (intra,) = kernel_call(
        intra_kernel, "v", [("v", (tokens, width), F32)], heads=heads
    )(queries, keys, values)
    stream, normed, send_rows = kernel_call(
        norm_kernel,
        "sv",
        [
            ("h", (tokens, width), F32),
            ("h", (tokens, width), BF16),
            ("h", (rows_n, width), BF16),
        ],
        [
            pltpu.VMEM((tokens, width), F32),
            pltpu.VMEM((tokens, width), BF16),
            pltpu.VMEM((rows_n, width), BF16),
            pltpu.SemaphoreType.DMA((groups + 2,)),
        ],
        heads=heads,
        groups=groups,
    )(i, queries, prefix, intra, residual_in, attn_gain[None], moe_gain[None], put)
    rows = exchange(send_rows.reshape(experts, slots, width)).reshape(rows_n, width)

    hidden, gated, delta, far_term = kernel_call(
        expert_kernel,
        "svh",
        [
            ("v", (rows_n, ff), BF16),
            ("v", (rows_n, ff), BF16),
            ("v", (rows_n, 2 * ff), BF16),
            ("v", (part, 3 * ff), BF16),
        ],
        [
            pltpu.VMEM((rows_n, width), BF16),
            pltpu.VMEM((rows_n, width + HD), BF16),
            pltpu.VMEM((len(got) + 1, part, 3 * ff), BF16),
            pltpu.SemaphoreType.DMA((groups + len(got) + 3 + pieces,)),
        ],
        groups=groups,
        gathered=len(got),
        pieces=pieces,
        slots=slots,
    )(me, turned, rows, *own, *got, *cots)
    expert_out, near_term, *terms = kernel_call(
        output_kernel,
        "svvvh",
        [("h", (rows_n, width), BF16), ("h", (part, 3 * ff), BF16)]
        + [("v", (part, 3 * ff), BF16)] * (groups - 2),
        [
            pltpu.VMEM((rows_n, width), BF16),
            pltpu.VMEM((rows_n, width + HD), BF16),
            pltpu.VMEM((len(got) + 1, part, ff), BF16),
            pltpu.VMEM((rows_n, width), BF16),
            pltpu.VMEM((part, 3 * ff), BF16),
            pltpu.SemaphoreType.DMA((groups + len(got) + 3 + pieces,)),
        ],
        groups=groups,
        gathered=len(got),
        pieces=pieces,
        slots=slots,
    )(me, hidden, gated, delta, rows, w_down, *got, *cots)
    terms = [terms[0], near_term, *terms[1:]]
    grads = kernel_call(total_kernel, "sv", [("v", (part, ff), F32)] * 3)(
        trainable, *scatter_xor(terms + [far_term], "dp")
    )

    back = exchange(expert_out.reshape(peers, slots, width)).reshape(rows_n, width)
    (mixed,) = kernel_call(
        combine_kernel, "sv", [("v", (1, tokens, width), BF16)], groups=groups
    )(i, stream, normed, router.T, expert_ids, slot, back)
    return (mixed, grads[0][None], grads[1][None], grads[2][None])


def solution(mesh):
    return jax.shard_map(
        layer,
        mesh=mesh,
        in_specs=(
            P("dp", "seq", None),
            P("dp", "seq", None),
            P("dp", "seq", None),
            P("dp", "seq", None),
            P("dp", "seq", None),
            P("dp", "seq", None),
            P(),
            P(),
            P(),
            P("seq", "dp", None),
            P("seq", "dp", None),
            P("seq", "dp", None),
            P("seq"),
        ),
        out_specs=(
            P("dp", "seq", None),
            P("seq", "dp", None),
            P("seq", "dp", None),
            P("seq", "dp", None),
        ),
        check_vma=False,
    )
```

```python
import functools

import jax
import jax.numpy as jnp
from jax import lax
from jax.experimental import pallas as pl
from jax.experimental.pallas import tpu as pltpu
from jax.sharding import PartitionSpec as P


HD = 128
F32 = jnp.float32
BF16 = jnp.bfloat16
MATMUL = (((1,), (0,)), ((), ()))
ROWS = (((0,), (0,)), ((), ()))
LANES = (((1,), (1,)), ((), ()))


def dot(a, b, dims=MATMUL):
    return lax.dot_general(a, b, dims, preferred_element_type=F32)


def kernel_call(body, ins, outs, scratch=(), flops=1_000_000_000, **static):
    place = {"s": pltpu.SMEM, "v": pltpu.VMEM, "h": pltpu.HBM}

    def call(*operands):
        letters = ins + ins[-1] * (len(operands) - len(ins))
        operands = [
            pltpu.with_memory_space_constraint(y, pltpu.HBM) if x == "h" else y
            for x, y in zip(letters, operands)
        ]
        return pl.pallas_call(
            functools.partial(body, **static),
            in_specs=[pl.BlockSpec(memory_space=place[x]) for x in letters],
            out_specs=[pl.BlockSpec(memory_space=place[x]) for x, _, _ in outs],
            out_shape=[
                (pltpu.HBM if x == "h" else jax.ShapeDtypeStruct)(shape, kind)
                for x, shape, kind in outs
            ],
            scratch_shapes=list(scratch),
            cost_estimate=pl.CostEstimate(flops=flops, bytes_accessed=4_000_000, transcendentals=0),
            compiler_params=pltpu.CompilerParams(vmem_limit_bytes=48 * 1024 * 1024),
        )(*operands)

    return call


class Copies:
    def __init__(self, sems):
        self.sems, self.n = sems, 0

    def start(self, source, target):
        copy = pltpu.make_async_copy(source, target, self.sems.at[self.n])
        self.n += 1
        copy.start()
        return copy


def route_kernel(
    i_ref, me_ref, ids_ref, cot_hbm, put_ref, slot_ref, *refs, groups, slots
):
    sends, (cot_ref, buf, sems) = refs[:-3], refs[-3:]
    tokens, rows_n = put_ref.shape
    width = cot_ref.shape[1]
    part = width // groups
    copies = Copies(sems)
    loads = []
    for d in range(groups):
        source = pl.multiple_of((i_ref[0] ^ d) * part, HD)
        loads.append(
            copies.start(
                cot_hbm.at[0, :, pl.ds(source, part)], cot_ref.at[:, pl.ds(d * part, part)]
            )
        )
    id_0, id_1 = ids_ref[0, :, 0:1], ids_ref[0, :, 1:2]
    lanes = lax.broadcasted_iota(jnp.int32, (tokens, HD), 1)
    hit_0, hit_1 = lanes == id_0, lanes == id_1
    count = jnp.where(hit_0, 1.0, jnp.where(hit_1, 1.0, 0.0)).astype(BF16)
    row = lax.broadcasted_iota(jnp.int32, (tokens, tokens), 0)
    col = lax.broadcasted_iota(jnp.int32, (tokens, tokens), 1)
    before = dot(jnp.where(row > col, 1.0, 0.0).astype(BF16), count)
    rank_0 = jnp.sum(jnp.where(hit_0, before, 0.0), axis=1, keepdims=True).astype(jnp.int32)
    rank_1 = jnp.sum(jnp.where(hit_1, before, 0.0), axis=1, keepdims=True).astype(jnp.int32)
    slot_0, slot_1 = id_0 * slots + rank_0, id_1 * slots + rank_1
    slot_ref[:, 0:1] = slot_0
    slot_ref[:, 1:2] = slot_1
    wide = lax.broadcasted_iota(jnp.int32, (tokens, rows_n), 1)
    put = jnp.where(wide == slot_0, 1.0, jnp.where(wide == slot_1, 1.0, 0.0)).astype(BF16)
    put_ref[...] = put
    both = jnp.broadcast_to((id_0 + id_1).astype(F32), (tokens, HD)).astype(BF16)
    buf[:, pl.ds(width, HD)] = dot(put, both, ROWS).astype(BF16)
    for d in range(groups):
        at = pl.ds(d * part, part)
        loads[d].wait()
        buf[:, at] = dot(put, cot_ref[:, at], ROWS).astype(BF16)
    if len(sends) == 1:
        stores = [copies.start(buf, sends[0])]
    else:
        stores = [
            copies.start(buf.at[pl.ds(pl.multiple_of((me_ref[0] ^ k) * slots, 16), slots)], send)
            for k, send in enumerate(sends)
        ]
    for copy in stores:
        copy.wait()


def load_rows(copies, me, pieces, target, slots):
    if len(pieces) == 1:
        return [copies.start(pieces[0], target)]
    return [
        copies.start(piece, target.at[pl.ds(pl.multiple_of((me ^ k) * slots, 16), slots)])
        for k, piece in enumerate(pieces)
    ]


def state_kernel(k_hbm, v_hbm, out_ref, k_ref, v_ref, sems, *, heads, chunks):
    copies = Copies(sems)
    size = heads // chunks
    loads = []
    for c in range(chunks):
        at = pl.ds(c * size * HD, size * HD)
        loads.append(
            [
                copies.start(k_hbm.at[0, :, at], k_ref.at[:, at]),
                copies.start(v_hbm.at[0, :, at], v_ref.at[:, at]),
            ]
        )
    for h in range(heads):
        if h % size == 0:
            for copy in loads[h // size]:
                copy.wait()
        at = pl.ds(h * HD, HD)
        out_ref[h] = dot(k_ref[:, at], v_ref[:, at], ROWS).astype(BF16)


def intra_kernel(q_ref, k_ref, v_ref, out_ref, *, heads):
    tokens = q_ref.shape[1]
    row = lax.broadcasted_iota(jnp.int32, (tokens, tokens), 0)
    col = lax.broadcasted_iota(jnp.int32, (tokens, tokens), 1)
    causal = row >= col
    for h in range(heads):
        at = pl.ds(h * HD, HD)
        scores = dot(q_ref[0, :, at], k_ref[0, :, at], LANES)
        scores = jnp.where(causal, scores, 0.0).astype(BF16)
        out_ref[:, at] = dot(scores, v_ref[0, :, at])


def norm_kernel(
    i_ref, q_ref, prefix_ref, intra_ref, residual_ref, attn_ref, moe_ref, put_ref,
    stream_out, normed_out, send_out, stream_ref, normed_ref, send_ref, sems, *, heads, groups,
):
    tokens, width = stream_ref.shape
    copies, started = Copies(sems), []
    squares = jnp.zeros((tokens, HD), F32)
    for h in range(heads):
        at = pl.ds(h * HD, HD)
        attended = intra_ref[:, at] + dot(q_ref[0, :, at], prefix_ref[h])
        mean = jnp.mean(attended * attended, axis=-1, keepdims=True)
        attended = attended * lax.rsqrt(mean + 1e-06)
        stream = residual_ref[0, :, at].astype(F32) + attended * attn_ref[:, at]
        stream_ref[:, at] = stream
        squares = squares + stream * stream
    scale = lax.rsqrt(jnp.sum(squares, axis=-1, keepdims=True) / width + 1e-06)
    part = width // groups
    for h in range(heads):
        at = pl.ds(h * HD, HD)
        normed_ref[:, at] = (stream_ref[:, at] * scale * moe_ref[:, at]).astype(BF16)
    put = put_ref[...]
    for d in range(groups):
        at = pl.ds(d * part, part)
        source = pl.multiple_of((i_ref[0] ^ d) * part, HD)
        send_ref[:, at] = dot(put, normed_ref[:, pl.ds(source, part)], ROWS).astype(BF16)
        started.append(copies.start(send_ref.at[:, at], send_out.at[:, at]))
    started.append(copies.start(normed_ref, normed_out))
    started.append(copies.start(stream_ref, stream_out))
    for copy in started:
        copy.wait()


def load_weights(copies, own, got, groups, target, cuts):
    loads = [[copies.start(x.at[0], target.at[0, :, c]) for x, c in zip(own, cuts[0])]]
    for d in range(1, groups):
        loads.append([copies.start(got[d - 1].at[:, cuts[1]], target.at[d])])
    return loads


def cot_kernel(me_ref, down_hbm, *refs, groups, pieces, slots):
    got, cots = refs[: groups - 1], refs[groups - 1 : groups - 1 + pieces]
    out_ref, tag_ref, cot_ref, w_ref, sems = refs[groups - 1 + pieces :]
    part, ff = w_ref.shape[1:]
    copies = Copies(sems)
    cot_loads = load_rows(copies, me_ref[0], cots, cot_ref, slots)
    cuts = ([pl.ds(0, ff)], pl.ds(2 * ff, ff))
    loads = load_weights(copies, [down_hbm], got, groups, w_ref, cuts)
    for copy in cot_loads + [x for load in loads for x in load]:
        copy.wait()
    total = dot(cot_ref[:, :part], w_ref[0])
    for d in range(1, groups):
        total = total + dot(cot_ref[:, pl.ds(d * part, part)], w_ref[d])
    out_ref[...] = total
    tag_ref[...] = cot_ref[:, pl.ds(cot_ref.shape[1] - HD, HD)].astype(F32)


def rows_kernel(me_ref, router_ref, tag_ref, rows_ref, gate_hbm, up_hbm, *refs, groups):
    got = refs[: groups - 1]
    out_ref, share_ref, w_ref, sems = refs[groups - 1 :]
    part = w_ref.shape[1]
    ff = w_ref.shape[2] // 2
    copies = Copies(sems)
    cuts = ([pl.ds(0, ff), pl.ds(ff, ff)], pl.ds(0, 2 * ff))
    loads = load_weights(copies, [gate_hbm, up_hbm], got, groups, w_ref, cuts)
    for copy in [x for load in loads for x in load]:
        copy.wait()
    total = dot(rows_ref[:, :part], w_ref[0])
    for d in range(1, groups):
        total = total + dot(rows_ref[:, pl.ds(d * part, part)], w_ref[d])
    out_ref[...] = total
    logits = dot(rows_ref[...], router_ref[...], LANES)
    lanes = lax.broadcasted_iota(jnp.int32, logits.shape, 1)
    me = me_ref[0]
    other = tag_ref[...].astype(jnp.int32)[:, : logits.shape[1]] - me
    sig = 1.0 / (1.0 + jnp.exp(-logits))
    own_sig = jnp.sum(jnp.where(lanes == me, sig, 0.0), axis=1, keepdims=True)
    other_sig = jnp.sum(jnp.where(lanes == other, sig, 0.0), axis=1, keepdims=True)
    share_ref[...] = jnp.broadcast_to(own_sig / (own_sig + other_sig), share_ref.shape)


def expert_kernel(
    me_ref, pre_ref, back_ref, share_ref, rows_ref, *refs, groups, last, pieces, slots
):
    got, cots = refs[:last], refs[last : last + pieces]
    hidden_ref, gated_ref, delta_ref, inner_ref, down_ref = refs[last + pieces : -2]
    cot_ref, sems = refs[-2:]
    part = cot_ref.shape[1]
    ff = hidden_ref.shape[1]
    copies = Copies(sems)
    at = pl.ds((groups - 1) * part, part)
    cot_loads = load_rows(copies, me_ref[0], [x.at[:, at] for x in cots], cot_ref, slots)
    mats = got[0][...] if last == 1 else got[0][...] + got[1][...]
    pre_gate = pre_ref[:, :ff] + dot(rows_ref[:, at], mats[:, :ff])
    pre_up = pre_ref[:, ff:] + dot(rows_ref[:, at], mats[:, ff : 2 * ff])
    gate = share_ref[:, 0:1]
    sigma = 1.0 / (1.0 + jnp.exp(-pre_gate))
    act = pre_gate * sigma
    hidden = act * pre_up
    hidden_ref[...] = hidden.astype(BF16)
    gated_ref[...] = (hidden * gate).astype(BF16)
    for copy in cot_loads:
        copy.wait()
    down_ref[...] = dot(cot_ref[...], gated_ref[...], ROWS).astype(BF16)
    d_hidden = (back_ref[...] + dot(cot_ref[...], mats[:, 2 * ff :])) * gate
    delta_ref[:, :ff] = (d_hidden * pre_up * sigma * (1.0 + pre_gate * (1.0 - sigma))).astype(BF16)
    delta_ref[:, ff:] = (d_hidden * act).astype(BF16)
    inner_ref[...] = dot(rows_ref[:, at], delta_ref[...], ROWS).astype(BF16)


def output_kernel(
    me_ref, hidden_ref, gated_ref, delta_ref, rows_ref, *refs, groups, last, pieces, slots
):
    late, refs = refs[:last], refs[last:]
    own, early, cots = refs[0], refs[1 : groups - 1], refs[groups - 1 : groups - 1 + pieces]
    out_hbm, *terms = refs[groups - 1 + pieces : -4]
    cot_ref, w_ref, out_ref, sems = refs[-4:]
    width = rows_ref.shape[1]
    part = width // groups
    ff = hidden_ref.shape[1]
    copies = Copies(sems)
    cot_loads = load_rows(copies, me_ref[0], cots, cot_ref, slots)
    cuts = ([pl.ds(0, ff)], pl.ds(2 * ff, ff))
    loads = load_weights(copies, [own], early, groups - 1, w_ref, cuts)
    for d in range(groups - 1):
        at = pl.ds(d * part, part)
        terms[2 * d + 1][...] = dot(rows_ref[:, at], delta_ref[...], ROWS).astype(BF16)
    for copy in cot_loads:
        copy.wait()
    for d in range(groups - 1):
        at = pl.ds(d * part, part)
        terms[2 * d][...] = dot(cot_ref[:, at], gated_ref[...], ROWS).astype(BF16)
    stores = []
    for d in range(groups):
        if d < groups - 1:
            for copy in loads[d]:
                copy.wait()
            mats = w_ref[d]
        else:
            mats = late[0][:, 2 * ff :]
            if last == 2:
                mats = mats + late[1][:, 2 * ff :]
        at = pl.ds(d * part, part)
        out_ref[:, at] = dot(hidden_ref[...], mats, LANES).astype(BF16)
        stores.append(copies.start(out_ref.at[:, at], out_hbm.at[:, at]))
    for copy in stores:
        copy.wait()


def combine_kernel(
    i_ref, stream_ref, normed_ref, router_ref, ids_ref, slot_ref, back_ref, out_ref, *, groups
):
    tokens, width = stream_ref.shape
    rows_n = back_ref.shape[0]
    logits = dot(normed_ref[...], router_ref[...], LANES)
    sig = 1.0 / (1.0 + jnp.exp(-logits))
    lanes = lax.broadcasted_iota(jnp.int32, logits.shape, 1)
    sig_0, sig_1 = (
        jnp.sum(jnp.where(lanes == ids_ref[0, :, j : j + 1], sig, 0.0), axis=1, keepdims=True)
        for j in range(2)
    )
    total = sig_0 + sig_1
    wide = lax.broadcasted_iota(jnp.int32, (tokens, rows_n), 1)
    take = jnp.where(
        wide == slot_ref[:, 0:1],
        sig_0 / total,
        jnp.where(wide == slot_ref[:, 1:2], sig_1 / total, 0.0),
    ).astype(BF16)
    part = width // groups
    for d in range(groups):
        at = pl.ds(pl.multiple_of((i_ref[0] ^ d) * part, HD), part)
        value = stream_ref[:, at] + dot(take, back_ref[:, pl.ds(d * part, part)])
        out_ref[0, :, at] = value.astype(BF16)


def total_kernel(scale_ref, *refs, outputs):
    parts, outs = refs[:-outputs], refs[-outputs:]
    ff = outs[0].shape[1]
    scale = jnp.where(scale_ref[0] > 0, 1.0, 0.0)
    for n, out in enumerate(outs):
        at = pl.ds(n * ff, ff)
        value = parts[0][:, at].astype(F32)
        for other in parts[1:]:
            value = value + other[:, at].astype(F32)
        out[...] = value * scale


def exclusive_prefix(local, axis):
    n, i = lax.axis_size(axis), lax.axis_index(axis)
    half = local.shape[0] // 2
    core = i % 2
    mine = lax.dynamic_slice_in_dim(local, core * half, half, 0)
    other = lax.dynamic_slice_in_dim(local, (1 - core) * half, half, 0)
    swap = [(j, j ^ 1) for j in range(n)]
    peer = lax.ppermute(other, axis, swap).astype(F32)
    mine = mine.astype(F32)
    total = (mine + peer).astype(BF16)
    before = jnp.zeros_like(mine)
    far = [lax.ppermute(total, axis, [(j, j + d) for j in range(n - d)]) for d in range(2, n, 2)]
    for got in far:
        before = before + got.astype(F32)
    own = before + jnp.where(core == 1, peer, 0.0)
    theirs = before + jnp.where(core == 0, mine, 0.0)
    back = lax.ppermute(theirs.astype(BF16), axis, swap)
    own = own.astype(BF16)
    return jnp.where(core == 0, jnp.concatenate([own, back], 0), jnp.concatenate([back, own], 0))


def send_xor(x, axis, d):
    return lax.ppermute(x, axis, [(j, j ^ d) for j in range(lax.axis_size(axis))])


ENDS = [(0, 1), (3, 2)]
MIDDLE = [(1, 2), (2, 1)]


def gather_xor(x, axis):
    n = lax.axis_size(axis)
    if n != 4:
        return [send_xor(x, axis, d) for d in range(1, n)]
    near, across = send_xor(x, axis, 1), send_xor(x, axis, 2)
    relayed = lax.ppermute(across, axis, [(b, a) for a, b in ENDS])
    middle = lax.ppermute(x, axis, MIDDLE)
    return [near, across, relayed, middle]


def scatter_xor(parts, axis):
    n = lax.axis_size(axis)
    if n != 4:
        return [parts[0]] + [send_xor(parts[d], axis, d) for d in range(1, n)]
    relayed = lax.ppermute(parts[3], axis, ENDS)
    middle = lax.ppermute(parts[3], axis, MIDDLE)
    merged = (parts[2].astype(F32) + relayed.astype(F32)).astype(BF16)
    across = send_xor(merged, axis, 2)
    near = send_xor(parts[1], axis, 1)
    return [parts[0], middle, across, near]


def exchange(x):
    return lax.all_to_all(x, "seq", split_axis=0, concat_axis=0, tiled=True)


def exchange_pieces(blocks):
    return [blocks[0]] + [
        send_xor(blocks[k], "seq", k) for k in range(len(blocks) - 1, 0, -1)
    ][::-1]


def swap_blocks(x, axis, dim):
    n, i = lax.axis_size(axis), lax.axis_index(axis)
    size = x.shape[dim] // n
    return jnp.concatenate(
        [lax.dynamic_slice_in_dim(x, (i ^ d) * size, size, dim) for d in range(n)], axis=dim
    )


def layer(
    queries,
    keys,
    values,
    residual_in,
    cotangent,
    expert_ids,
    router,
    attn_gain,
    moe_gain,
    w_gate,
    w_up,
    w_down,
    trainable,
):
    tokens = queries.shape[1]
    width = queries.shape[2]
    heads = width // HD
    experts = router.shape[1]
    peers = lax.axis_size("seq")
    groups = lax.axis_size("dp")
    slots = max(2, 3 * tokens // peers)
    rows_n = experts * slots
    part = width // groups
    ff = w_gate.shape[2]
    i = lax.axis_index("dp")[None]
    me = lax.axis_index("seq")[None]
    turned = swap_blocks(router.T, "dp", 1)

    split = slots % 16 == 0
    cot_shape = (slots if split else rows_n, width + HD)
    pieces = peers if split else 1
    put, slot, *cot_send = kernel_call(
        route_kernel,
        "ssvh",
        [("v", (tokens, rows_n), BF16), ("v", (tokens, 2), jnp.int32)]
        + [("h", cot_shape, BF16)] * pieces,
        [
            pltpu.VMEM((tokens, width), BF16),
            pltpu.VMEM((rows_n, width + HD), BF16),
            pltpu.SemaphoreType.DMA((groups + pieces,)),
        ],
        groups=groups,
        slots=slots,
    )(i, me, expert_ids, cotangent)
    if split:
        cots = exchange_pieces(cot_send)
    else:
        cots = [exchange(cot_send[0].reshape(experts, slots, -1)).reshape(cot_shape)]

    got = gather_xor(jnp.concatenate([w_gate[0], w_up[0], w_down[0]], axis=1), "dp")

    (local,) = kernel_call(
        state_kernel,
        "h",
        [("v", (heads, HD, HD), BF16)],
        [
            pltpu.VMEM((tokens, width), BF16),
            pltpu.VMEM((tokens, width), BF16),
            pltpu.SemaphoreType.DMA((8,)),
        ],
        heads=heads,
        chunks=4,
    )(keys, values)
    prefix = exclusive_prefix(local, "seq")

    (intra,) = kernel_call(
        intra_kernel, "v", [("v", (tokens, width), F32)], heads=heads
    )(queries, keys, values)
    stream, normed, send_rows = kernel_call(
        norm_kernel,
        "sv",
        [
            ("h", (tokens, width), F32),
            ("h", (tokens, width), BF16),
            ("h", (rows_n, width), BF16),
        ],
        [
            pltpu.VMEM((tokens, width), F32),
            pltpu.VMEM((tokens, width), BF16),
            pltpu.VMEM((rows_n, width), BF16),
            pltpu.SemaphoreType.DMA((groups + 2,)),
        ],
        heads=heads,
        groups=groups,
    )(i, queries, prefix, intra, residual_in, attn_gain[None], moe_gain[None], put)
    rows = exchange(send_rows.reshape(experts, slots, width)).reshape(rows_n, width)

    early = got[: groups - 2]
    late = got[groups - 2 :]
    cot_part, tags = kernel_call(
        cot_kernel,
        "sh",
        [("v", (rows_n, ff), F32), ("v", (rows_n, HD), F32)],
        [
            pltpu.VMEM((rows_n, width + HD), BF16),
            pltpu.VMEM((groups - 1, part, ff), BF16),
            pltpu.SemaphoreType.DMA((groups + pieces,)),
        ],
        groups=groups - 1,
        pieces=pieces,
        slots=slots,
    )(me, w_down, *early, *cots)
    row_part, share = kernel_call(
        rows_kernel,
        "svvvh",
        [("v", (rows_n, 2 * ff), F32), ("v", (rows_n, HD), F32)],
        [
            pltpu.VMEM((groups - 1, part, 2 * ff), BF16),
            pltpu.SemaphoreType.DMA((groups + 1,)),
        ],
        groups=groups - 1,
    )(me, turned, tags, rows, w_gate, w_up, *early)
    hidden, gated, delta, far_inner, far_down = kernel_call(
        expert_kernel,
        "svvvv" + "v" * len(late) + "h",
        [
            ("v", (rows_n, ff), BF16),
            ("v", (rows_n, ff), BF16),
            ("v", (rows_n, 2 * ff), BF16),
            ("v", (part, 2 * ff), BF16),
            ("v", (part, ff), BF16),
        ],
        [
            pltpu.VMEM((rows_n, part), BF16),
            pltpu.SemaphoreType.DMA((pieces,)),
        ],
        groups=groups,
        last=len(late),
        pieces=pieces,
        slots=slots,
    )(me, row_part, cot_part, share, rows, *late, *cots)
    expert_out, *terms = kernel_call(
        output_kernel,
        "svvvv" + "v" * len(late) + "h",
        [("h", (rows_n, width), BF16)]
        + [("v", (part, ff), BF16), ("v", (part, 2 * ff), BF16)] * (groups - 1),
        [
            pltpu.VMEM((rows_n, width + HD), BF16),
            pltpu.VMEM((groups - 1, part, ff), BF16),
            pltpu.VMEM((rows_n, width), BF16),
            pltpu.SemaphoreType.DMA((2 * groups + pieces,)),
        ],
        groups=groups,
        last=len(late),
        pieces=pieces,
        slots=slots,
    )(me, hidden, gated, delta, rows, *late, w_down, *early, *cots)
    down_parts = scatter_xor(terms[0::2] + [far_down], "dp")
    inner_parts = scatter_xor(terms[1::2] + [far_inner], "dp")
    back = exchange(expert_out.reshape(peers, slots, width)).reshape(rows_n, width)
    (mixed,) = kernel_call(
        combine_kernel, "sv", [("v", (1, tokens, width), BF16)], groups=groups
    )(i, stream, normed, router.T, expert_ids, slot, back)
    mixed, *inner_parts = lax.optimization_barrier((mixed, *inner_parts))
    (grad_down,) = kernel_call(
        total_kernel, "sv", [("v", (part, ff), F32)], outputs=1
    )(trainable, *down_parts)
    grad_gate, grad_up = kernel_call(
        total_kernel, "sv", [("v", (part, ff), F32)] * 2, outputs=2
    )(trainable, *inner_parts)
    return (mixed, grad_gate[None], grad_up[None], grad_down[None])


def solution(mesh):
    return jax.shard_map(
        layer,
        mesh=mesh,
        in_specs=(
            P("dp", "seq", None),
            P("dp", "seq", None),
            P("dp", "seq", None),
            P("dp", "seq", None),
            P("dp", "seq", None),
            P("dp", "seq", None),
            P(),
            P(),
            P(),
            P("seq", "dp", None),
            P("seq", "dp", None),
            P("seq", "dp", None),
            P("seq"),
        ),
        out_specs=(
            P("dp", "seq", None),
            P("seq", "dp", None),
            P("seq", "dp", None),
            P("seq", "dp", None),
        ),
        check_vma=False,
    )
```

```python
import functools

import jax
import jax.numpy as jnp
from jax import lax
from jax.experimental import pallas as pl
from jax.experimental.pallas import tpu as pltpu
from jax.sharding import PartitionSpec as P


HD = 128
F32 = jnp.float32
BF16 = jnp.bfloat16
MATMUL = (((1,), (0,)), ((), ()))
ROWS = (((0,), (0,)), ((), ()))
LANES = (((1,), (1,)), ((), ()))


def dot(a, b, dims=MATMUL):
    return lax.dot_general(a, b, dims, preferred_element_type=F32)


def kernel_call(body, ins, outs, scratch=(), flops=1_000_000_000, **static):
    place = {"s": pltpu.SMEM, "v": pltpu.VMEM, "h": pltpu.HBM}

    def call(*operands):
        letters = ins + ins[-1] * (len(operands) - len(ins))
        operands = [
            pltpu.with_memory_space_constraint(y, pltpu.HBM) if x == "h" else y
            for x, y in zip(letters, operands)
        ]
        return pl.pallas_call(
            functools.partial(body, **static),
            in_specs=[pl.BlockSpec(memory_space=place[x]) for x in letters],
            out_specs=[pl.BlockSpec(memory_space=place[x]) for x, _, _ in outs],
            out_shape=[
                (pltpu.HBM if x == "h" else jax.ShapeDtypeStruct)(shape, kind)
                for x, shape, kind in outs
            ],
            scratch_shapes=list(scratch),
            cost_estimate=pl.CostEstimate(flops=flops, bytes_accessed=4_000_000, transcendentals=0),
            compiler_params=pltpu.CompilerParams(vmem_limit_bytes=24 * 1024 * 1024),
        )(*operands)

    return call


def block_at(i, d, n):
    if n != 4 or d in (0, 3):
        return i ^ d
    inside = ((i >> 1) ^ i) & 1
    return i ^ (1 + inside if d == 1 else 2 - inside)


class Copies:
    def __init__(self, sems):
        self.sems, self.n = sems, 0

    def start(self, source, target):
        copy = pltpu.make_async_copy(source, target, self.sems.at[self.n])
        self.n += 1
        copy.start()
        return copy


def route_kernel(
    i_ref, me_ref, ids_ref, cot_hbm, put_ref, slot_ref, *refs, groups, slots
):
    sends, (cot_ref, buf, sems) = refs[:-3], refs[-3:]
    tokens, rows_n = put_ref.shape
    width = cot_ref.shape[1]
    part = width // groups
    copies = Copies(sems)
    loads = []
    for d in range(groups):
        source = pl.multiple_of(block_at(i_ref[0], d, groups) * part, HD)
        loads.append(
            copies.start(
                cot_hbm.at[0, :, pl.ds(source, part)], cot_ref.at[:, pl.ds(d * part, part)]
            )
        )
    id_0, id_1 = ids_ref[0, :, 0:1], ids_ref[0, :, 1:2]
    lanes = lax.broadcasted_iota(jnp.int32, (tokens, HD), 1)
    hit_0, hit_1 = lanes == id_0, lanes == id_1
    count = jnp.where(hit_0, 1.0, jnp.where(hit_1, 1.0, 0.0)).astype(BF16)
    row = lax.broadcasted_iota(jnp.int32, (tokens, tokens), 0)
    col = lax.broadcasted_iota(jnp.int32, (tokens, tokens), 1)
    before = dot(jnp.where(row > col, 1.0, 0.0).astype(BF16), count)
    rank_0 = jnp.sum(jnp.where(hit_0, before, 0.0), axis=1, keepdims=True).astype(jnp.int32)
    rank_1 = jnp.sum(jnp.where(hit_1, before, 0.0), axis=1, keepdims=True).astype(jnp.int32)
    slot_0, slot_1 = id_0 * slots + rank_0, id_1 * slots + rank_1
    slot_ref[:, 0:1] = slot_0
    slot_ref[:, 1:2] = slot_1
    wide = lax.broadcasted_iota(jnp.int32, (tokens, rows_n), 1)
    put = jnp.where(wide == slot_0, 1.0, jnp.where(wide == slot_1, 1.0, 0.0)).astype(BF16)
    put_ref[...] = put
    both = jnp.broadcast_to((id_0 + id_1).astype(F32), (tokens, HD)).astype(BF16)
    buf[:, pl.ds(width, HD)] = dot(put, both, ROWS).astype(BF16)
    for d in range(groups):
        at = pl.ds(d * part, part)
        loads[d].wait()
        buf[:, at] = dot(put, cot_ref[:, at], ROWS).astype(BF16)
    if len(sends) == 1:
        stores = [copies.start(buf, sends[0])]
    else:
        stores = [
            copies.start(buf.at[pl.ds(pl.multiple_of((me_ref[0] ^ k) * slots, 16), slots)], send)
            for k, send in enumerate(sends)
        ]
    for copy in stores:
        copy.wait()


def load_rows(copies, me, pieces, target, slots):
    if len(pieces) == 1:
        return [copies.start(pieces[0], target)]
    return [
        copies.start(piece, target.at[pl.ds(pl.multiple_of((me ^ k) * slots, 16), slots)])
        for k, piece in enumerate(pieces)
    ]


def state_kernel(k_hbm, v_hbm, out_ref, k_ref, v_ref, sems, *, heads, chunks):
    copies = Copies(sems)
    size = heads // chunks
    loads = []
    for c in range(chunks):
        at = pl.ds(c * size * HD, size * HD)
        loads.append(
            [
                copies.start(k_hbm.at[0, :, at], k_ref.at[:, at]),
                copies.start(v_hbm.at[0, :, at], v_ref.at[:, at]),
            ]
        )
    for h in range(heads):
        if h % size == 0:
            for copy in loads[h // size]:
                copy.wait()
        at = pl.ds(h * HD, HD)
        out_ref[h] = dot(k_ref[:, at], v_ref[:, at], ROWS).astype(BF16)


def intra_kernel(q_ref, k_ref, v_ref, out_ref, *, heads):
    tokens = q_ref.shape[1]
    row = lax.broadcasted_iota(jnp.int32, (tokens, tokens), 0)
    col = lax.broadcasted_iota(jnp.int32, (tokens, tokens), 1)
    causal = row >= col
    for h in range(heads):
        at = pl.ds(h * HD, HD)
        scores = dot(q_ref[0, :, at], k_ref[0, :, at], LANES)
        scores = jnp.where(causal, scores, 0.0).astype(BF16)
        out_ref[:, at] = dot(scores, v_ref[0, :, at])


def norm_kernel(
    i_ref, q_ref, prefix_ref, intra_ref, residual_ref, attn_ref, moe_ref, put_ref,
    stream_out, normed_out, send_out, stream_ref, normed_ref, send_ref, sems, *, heads, groups,
):
    tokens, width = stream_ref.shape
    copies, started = Copies(sems), []
    squares = jnp.zeros((tokens, HD), F32)
    for h in range(heads):
        at = pl.ds(h * HD, HD)
        attended = intra_ref[:, at] + dot(q_ref[0, :, at], prefix_ref[h])
        mean = jnp.mean(attended * attended, axis=-1, keepdims=True)
        attended = attended * lax.rsqrt(mean + 1e-06)
        stream = residual_ref[0, :, at].astype(F32) + attended * attn_ref[:, at]
        stream_ref[:, at] = stream
        squares = squares + stream * stream
    scale = lax.rsqrt(jnp.sum(squares, axis=-1, keepdims=True) / width + 1e-06)
    part = width // groups
    for h in range(heads):
        at = pl.ds(h * HD, HD)
        normed_ref[:, at] = (stream_ref[:, at] * scale * moe_ref[:, at]).astype(BF16)
    put = put_ref[...]
    for d in range(groups):
        at = pl.ds(d * part, part)
        source = pl.multiple_of(block_at(i_ref[0], d, groups) * part, HD)
        send_ref[:, at] = dot(put, normed_ref[:, pl.ds(source, part)], ROWS).astype(BF16)
        started.append(copies.start(send_ref.at[:, at], send_out.at[:, at]))
    started.append(copies.start(normed_ref, normed_out))
    started.append(copies.start(stream_ref, stream_out))
    for copy in started:
        copy.wait()


def load_weights(copies, own, got, groups, target, cuts):
    loads = [[copies.start(x.at[0], target.at[0, :, c]) for x, c in zip(own, cuts[0])]]
    for d in range(1, groups):
        loads.append([copies.start(got[d - 1].at[:, cuts[1]], target.at[d])])
    return loads


def cot_kernel(me_ref, down_hbm, *refs, groups, pieces, slots):
    got, cots = refs[: groups - 1], refs[groups - 1 : groups - 1 + pieces]
    out_ref, tag_hbm, cot_ref, tag_ref, w_ref, sems = refs[groups - 1 + pieces :]
    part, ff = w_ref.shape[1:]
    copies = Copies(sems)
    cot_loads = load_rows(copies, me_ref[0], cots, cot_ref, slots)
    cuts = ([pl.ds(0, ff)], pl.ds(2 * ff, ff))
    loads = load_weights(copies, [down_hbm], got, groups, w_ref, cuts)
    for copy in cot_loads:
        copy.wait()
    tag_ref[...] = cot_ref[:, pl.ds(cot_ref.shape[1] - HD, HD)].astype(F32)
    store = copies.start(tag_ref, tag_hbm)
    for copy in [x for load in loads for x in load]:
        copy.wait()
    total = dot(cot_ref[:, :part], w_ref[0])
    for d in range(1, groups):
        total = total + dot(cot_ref[:, pl.ds(d * part, part)], w_ref[d])
    out_ref[...] = total
    store.wait()


def rows_kernel(me_ref, rows_ref, router_hbm, tag_hbm, gate_hbm, up_hbm, *refs, groups):
    got = refs[: groups - 1]
    out_ref, share_ref, router_ref, tag_ref, w_ref, sems = refs[groups - 1 :]
    part = w_ref.shape[1]
    ff = w_ref.shape[2] // 2
    copies = Copies(sems)
    router_load = copies.start(router_hbm, router_ref)
    cuts = ([pl.ds(0, ff), pl.ds(ff, ff)], pl.ds(0, 2 * ff))
    loads = load_weights(copies, [gate_hbm, up_hbm], got, groups, w_ref, cuts)
    tag_load = copies.start(tag_hbm, tag_ref)
    router_load.wait()
    logits = dot(rows_ref[...], router_ref[...], LANES)
    total = None
    for d in range(groups):
        for copy in loads[d]:
            copy.wait()
        value = dot(rows_ref[:, pl.ds(d * part, part)], w_ref[d])
        total = value if total is None else total + value
    out_ref[...] = total
    tag_load.wait()
    lanes = lax.broadcasted_iota(jnp.int32, logits.shape, 1)
    me = me_ref[0]
    other = tag_ref[...].astype(jnp.int32)[:, : logits.shape[1]] - me
    sig = 1.0 / (1.0 + jnp.exp(-logits))
    own_sig = jnp.sum(jnp.where(lanes == me, sig, 0.0), axis=1, keepdims=True)
    other_sig = jnp.sum(jnp.where(lanes == other, sig, 0.0), axis=1, keepdims=True)
    share_ref[...] = jnp.broadcast_to(own_sig / (own_sig + other_sig), share_ref.shape)


def expert_kernel(
    me_ref, pre_ref, back_ref, share_ref, rows_ref, *refs, groups, last, pieces, slots
):
    got, cots = refs[:last], refs[last : last + pieces]
    hidden_ref, gated_ref, delta_ref, inner_ref, down_ref = refs[last + pieces : -2]
    cot_ref, sems = refs[-2:]
    part = cot_ref.shape[1]
    ff = hidden_ref.shape[1]
    copies = Copies(sems)
    at = pl.ds((groups - 1) * part, part)
    cot_loads = load_rows(copies, me_ref[0], [x.at[:, at] for x in cots], cot_ref, slots)
    mats = got[0][...] if last == 1 else got[0][...] + got[1][...]
    pre_gate = pre_ref[:, :ff] + dot(rows_ref[:, at], mats[:, :ff])
    pre_up = pre_ref[:, ff:] + dot(rows_ref[:, at], mats[:, ff : 2 * ff])
    gate = share_ref[:, 0:1]
    sigma = 1.0 / (1.0 + jnp.exp(-pre_gate))
    act = pre_gate * sigma
    hidden = act * pre_up
    hidden_ref[...] = hidden.astype(BF16)
    gated_ref[...] = (hidden * gate).astype(BF16)
    for copy in cot_loads:
        copy.wait()
    down_ref[...] = dot(cot_ref[...], gated_ref[...], ROWS).astype(BF16)
    d_hidden = (back_ref[...] + dot(cot_ref[...], mats[:, 2 * ff :])) * gate
    delta_ref[:, :ff] = (d_hidden * pre_up * sigma * (1.0 + pre_gate * (1.0 - sigma))).astype(BF16)
    delta_ref[:, ff:] = (d_hidden * act).astype(BF16)
    inner_ref[...] = dot(rows_ref[:, at], delta_ref[...], ROWS).astype(BF16)


def output_kernel(
    me_ref, hidden_ref, gated_ref, delta_ref, rows_ref, *refs, groups, last, pieces, slots
):
    late, refs = refs[:last], refs[last:]
    own, early, cots = refs[0], refs[1 : groups - 1], refs[groups - 1 : groups - 1 + pieces]
    out_hbm, *terms = refs[groups - 1 + pieces : -4]
    cot_ref, w_ref, out_ref, sems = refs[-4:]
    width = rows_ref.shape[1]
    part = width // groups
    ff = hidden_ref.shape[1]
    copies = Copies(sems)
    cot_loads = load_rows(copies, me_ref[0], cots, cot_ref, slots)
    cuts = ([pl.ds(0, ff)], pl.ds(2 * ff, ff))
    loads = load_weights(copies, [own], early, groups - 1, w_ref, cuts)
    for d in range(groups - 1):
        at = pl.ds(d * part, part)
        terms[2 * d + 1][...] = dot(rows_ref[:, at], delta_ref[...], ROWS).astype(BF16)
    for copy in cot_loads:
        copy.wait()
    for d in range(groups - 1):
        at = pl.ds(d * part, part)
        terms[2 * d][...] = dot(cot_ref[:, at], gated_ref[...], ROWS).astype(BF16)
    stores = []
    for d in range(groups):
        if d < groups - 1:
            for copy in loads[d]:
                copy.wait()
            mats = w_ref[d]
        else:
            mats = late[0][:, 2 * ff :]
            if last == 2:
                mats = mats + late[1][:, 2 * ff :]
        at = pl.ds(d * part, part)
        out_ref[:, at] = dot(hidden_ref[...], mats, LANES).astype(BF16)
        stores.append(copies.start(out_ref.at[:, at], out_hbm.at[:, at]))
    for copy in stores:
        copy.wait()


def combine_kernel(
    i_ref, stream_ref, normed_ref, router_ref, ids_ref, slot_ref, back_ref, out_ref, *, groups
):
    tokens, width = stream_ref.shape
    rows_n = back_ref.shape[0]
    logits = dot(normed_ref[...], router_ref[...], LANES)
    sig = 1.0 / (1.0 + jnp.exp(-logits))
    lanes = lax.broadcasted_iota(jnp.int32, logits.shape, 1)
    sig_0, sig_1 = (
        jnp.sum(jnp.where(lanes == ids_ref[0, :, j : j + 1], sig, 0.0), axis=1, keepdims=True)
        for j in range(2)
    )
    total = sig_0 + sig_1
    wide = lax.broadcasted_iota(jnp.int32, (tokens, rows_n), 1)
    take = jnp.where(
        wide == slot_ref[:, 0:1],
        sig_0 / total,
        jnp.where(wide == slot_ref[:, 1:2], sig_1 / total, 0.0),
    ).astype(BF16)
    part = width // groups
    for d in range(groups):
        at = pl.ds(pl.multiple_of(block_at(i_ref[0], d, groups) * part, HD), part)
        value = stream_ref[:, at] + dot(take, back_ref[:, pl.ds(d * part, part)])
        out_ref[0, :, at] = value.astype(BF16)


def total_kernel(scale_ref, *refs, outputs, parts_n, chunks):
    parts, outs = refs[:parts_n], refs[parts_n : parts_n + outputs]
    part_ref, out_ref, sems = refs[parts_n + outputs :]
    copies = Copies(sems)
    rows_n = out_ref.shape[0]
    size = rows_n // chunks
    ff = outs[0].shape[1]
    scale = jnp.where(scale_ref[0] > 0, 1.0, 0.0)
    loads, stores = [], []
    for c in range(chunks):
        at = pl.ds(c * size, size)
        loads.append([copies.start(x.at[at], part_ref.at[n, at]) for n, x in enumerate(parts)])
    for c in range(chunks):
        at = pl.ds(c * size, size)
        for copy in loads[c]:
            copy.wait()
        value = part_ref[0, at].astype(F32)
        for n in range(1, parts_n):
            value = value + part_ref[n, at].astype(F32)
        out_ref[at] = value * scale
        for n, out in enumerate(outs):
            stores.append(copies.start(out_ref.at[at, pl.ds(n * ff, ff)], out.at[at]))
    for copy in stores:
        copy.wait()


def total_call(trainable, parts, outputs):
    rows_n, columns = parts[0].shape
    chunks = 4
    return kernel_call(
        total_kernel,
        "sh",
        [("h", (rows_n, columns // outputs), F32)] * outputs,
        [
            pltpu.VMEM((len(parts), rows_n, columns), BF16),
            pltpu.VMEM((rows_n, columns), F32),
            pltpu.SemaphoreType.DMA((chunks * (len(parts) + outputs),)),
        ],
        outputs=outputs,
        parts_n=len(parts),
        chunks=chunks,
    )(trainable, *parts)


def exclusive_prefix(local, axis):
    n, i = lax.axis_size(axis), lax.axis_index(axis)
    half = local.shape[0] // 2
    core = i % 2
    mine = lax.dynamic_slice_in_dim(local, core * half, half, 0)
    other = lax.dynamic_slice_in_dim(local, (1 - core) * half, half, 0)
    swap = [(j, j ^ 1) for j in range(n)]
    peer = lax.ppermute(other, axis, swap).astype(F32)
    mine = mine.astype(F32)
    total = (mine + peer).astype(BF16)
    before = jnp.zeros_like(mine)
    far = [lax.ppermute(total, axis, [(j, j + d) for j in range(n - d)]) for d in range(2, n, 2)]
    for got in far:
        before = before + got.astype(F32)
    own = before + jnp.where(core == 1, peer, 0.0)
    theirs = before + jnp.where(core == 0, mine, 0.0)
    back = lax.ppermute(theirs.astype(BF16), axis, swap)
    own = own.astype(BF16)
    return jnp.where(core == 0, jnp.concatenate([own, back], 0), jnp.concatenate([back, own], 0))


def send_xor(x, axis, d):
    return lax.ppermute(x, axis, [(j, j ^ d) for j in range(lax.axis_size(axis))])


ENDS = [(0, 1), (3, 2)]
MIDDLE = [(1, 2), (2, 1)]
FIRST = [(0, 2), (3, 1), (1, 0), (2, 3)]
SECOND = [(1, 3), (2, 0), (0, 1), (3, 2)]


def gather_line(x, axis):
    n = lax.axis_size(axis)
    if n != 4:
        return [send_xor(x, axis, d) for d in range(1, n)]
    first = lax.ppermute(x, axis, FIRST)
    second = lax.ppermute(x, axis, SECOND)
    relayed = lax.ppermute(first, axis, [(b, a) for a, b in ENDS])
    middle = lax.ppermute(x, axis, MIDDLE)
    return [first, second, relayed, middle]


def scatter_line(parts, axis):
    n = lax.axis_size(axis)
    if n != 4:
        return [parts[0]] + [send_xor(parts[d], axis, d) for d in range(1, n)]
    relayed = lax.ppermute(parts[3], axis, ENDS)
    middle = lax.ppermute(parts[3], axis, MIDDLE)
    second = lax.ppermute(parts[2], axis, [(b, a) for a, b in SECOND])
    merged = (parts[1].astype(F32) + relayed.astype(F32)).astype(BF16)
    first = lax.ppermute(merged, axis, [(b, a) for a, b in FIRST])
    return [parts[0], middle, second, first]


def exchange(x):
    return lax.all_to_all(x, "seq", split_axis=0, concat_axis=0, tiled=True)


def exchange_pieces(blocks):
    return [blocks[0]] + [
        send_xor(blocks[k], "seq", k) for k in range(len(blocks) - 1, 0, -1)
    ][::-1]


def swap_blocks(x, axis, dim):
    n, i = lax.axis_size(axis), lax.axis_index(axis)
    size = x.shape[dim] // n
    return jnp.concatenate(
        [lax.dynamic_slice_in_dim(x, block_at(i, d, n) * size, size, dim) for d in range(n)], axis=dim
    )


def layer(
    queries,
    keys,
    values,
    residual_in,
    cotangent,
    expert_ids,
    router,
    attn_gain,
    moe_gain,
    w_gate,
    w_up,
    w_down,
    trainable,
):
    tokens = queries.shape[1]
    width = queries.shape[2]
    heads = width // HD
    experts = router.shape[1]
    peers = lax.axis_size("seq")
    groups = lax.axis_size("dp")
    slots = max(2, 3 * tokens // peers)
    rows_n = experts * slots
    part = width // groups
    ff = w_gate.shape[2]
    i = lax.axis_index("dp")[None]
    me = lax.axis_index("seq")[None]
    turned = swap_blocks(router.T, "dp", 1)

    split = slots % 16 == 0
    cot_shape = (slots if split else rows_n, width + HD)
    pieces = peers if split else 1
    put, slot, *cot_send = kernel_call(
        route_kernel,
        "ssvh",
        [("v", (tokens, rows_n), BF16), ("v", (tokens, 2), jnp.int32)]
        + [("h", cot_shape, BF16)] * pieces,
        [
            pltpu.VMEM((tokens, width), BF16),
            pltpu.VMEM((rows_n, width + HD), BF16),
            pltpu.SemaphoreType.DMA((groups + pieces,)),
        ],
        groups=groups,
        slots=slots,
    )(i, me, expert_ids, cotangent)
    if split:
        cots = exchange_pieces(cot_send)
    else:
        cots = [exchange(cot_send[0].reshape(experts, slots, -1)).reshape(cot_shape)]

    got = gather_line(jnp.concatenate([w_gate[0], w_up[0], w_down[0]], axis=1), "dp")

    (local,) = kernel_call(
        state_kernel,
        "h",
        [("v", (heads, HD, HD), BF16)],
        [
            pltpu.VMEM((tokens, width), BF16),
            pltpu.VMEM((tokens, width), BF16),
            pltpu.SemaphoreType.DMA((8,)),
        ],
        heads=heads,
        chunks=4,
    )(keys, values)
    prefix = exclusive_prefix(local, "seq")

    (intra,) = kernel_call(
        intra_kernel, "v", [("v", (tokens, width), F32)], heads=heads
    )(queries, keys, values)
    stream, normed, send_rows = kernel_call(
        norm_kernel,
        "sv",
        [
            ("h", (tokens, width), F32),
            ("h", (tokens, width), BF16),
            ("h", (rows_n, width), BF16),
        ],
        [
            pltpu.VMEM((tokens, width), F32),
            pltpu.VMEM((tokens, width), BF16),
            pltpu.VMEM((rows_n, width), BF16),
            pltpu.SemaphoreType.DMA((groups + 2,)),
        ],
        heads=heads,
        groups=groups,
    )(i, queries, prefix, intra, residual_in, attn_gain[None], moe_gain[None], put)
    rows = exchange(send_rows.reshape(experts, slots, width)).reshape(rows_n, width)

    early = got[: groups - 2]
    late = got[groups - 2 :]
    cot_part, tags = kernel_call(
        cot_kernel,
        "sh",
        [("v", (rows_n, ff), F32), ("h", (rows_n, HD), F32)],
        [
            pltpu.VMEM((rows_n, width + HD), BF16),
            pltpu.VMEM((rows_n, HD), F32),
            pltpu.VMEM((groups - 1, part, ff), BF16),
            pltpu.SemaphoreType.DMA((groups + 1 + pieces,)),
        ],
        groups=groups - 1,
        pieces=pieces,
        slots=slots,
    )(me, w_down, *early, *cots)
    row_part, share = kernel_call(
        rows_kernel,
        "svh",
        [("v", (rows_n, 2 * ff), F32), ("v", (rows_n, HD), F32)],
        [
            pltpu.VMEM((experts, width), BF16),
            pltpu.VMEM((rows_n, HD), F32),
            pltpu.VMEM((groups - 1, part, 2 * ff), BF16),
            pltpu.SemaphoreType.DMA((groups + 2,)),
        ],
        groups=groups - 1,
    )(me, rows, turned, tags, w_gate, w_up, *early)
    hidden, gated, delta, far_inner, far_down = kernel_call(
        expert_kernel,
        "svvvv" + "v" * len(late) + "h",
        [
            ("v", (rows_n, ff), BF16),
            ("v", (rows_n, ff), BF16),
            ("v", (rows_n, 2 * ff), BF16),
            ("v", (part, 2 * ff), BF16),
            ("v", (part, ff), BF16),
        ],
        [
            pltpu.VMEM((rows_n, part), BF16),
            pltpu.SemaphoreType.DMA((pieces,)),
        ],
        groups=groups,
        last=len(late),
        pieces=pieces,
        slots=slots,
    )(me, row_part, cot_part, share, rows, *late, *cots)
    expert_out, *terms = kernel_call(
        output_kernel,
        "svvvv" + "v" * len(late) + "h",
        [("h", (rows_n, width), BF16)]
        + [("v", (part, ff), BF16), ("v", (part, 2 * ff), BF16)] * (groups - 1),
        [
            pltpu.VMEM((rows_n, width + HD), BF16),
            pltpu.VMEM((groups - 1, part, ff), BF16),
            pltpu.VMEM((rows_n, width), BF16),
            pltpu.SemaphoreType.DMA((2 * groups + pieces,)),
        ],
        groups=groups,
        last=len(late),
        pieces=pieces,
        slots=slots,
    )(me, hidden, gated, delta, rows, *late, w_down, *early, *cots)
    down_parts = scatter_line(terms[0::2] + [far_down], "dp")
    inner_parts = scatter_line(terms[1::2] + [far_inner], "dp")
    back = exchange(expert_out.reshape(peers, slots, width)).reshape(rows_n, width)
    (mixed,) = kernel_call(
        combine_kernel, "sv", [("v", (1, tokens, width), BF16)], groups=groups
    )(i, stream, normed, router.T, expert_ids, slot, back)
    mixed, *inner_parts = lax.optimization_barrier((mixed, *inner_parts))
    (grad_down,) = total_call(trainable, down_parts, 1)
    grad_gate, grad_up = total_call(trainable, inner_parts, 2)
    return (mixed, grad_gate[None], grad_up[None], grad_down[None])


def solution(mesh):
    return jax.shard_map(
        layer,
        mesh=mesh,
        in_specs=(
            P("dp", "seq", None),
            P("dp", "seq", None),
            P("dp", "seq", None),
            P("dp", "seq", None),
            P("dp", "seq", None),
            P("dp", "seq", None),
            P(),
            P(),
            P(),
            P("seq", "dp", None),
            P("seq", "dp", None),
            P("seq", "dp", None),
            P("seq"),
        ),
        out_specs=(
            P("dp", "seq", None),
            P("seq", "dp", None),
            P("seq", "dp", None),
            P("seq", "dp", None),
        ),
        check_vma=False,
    )
```

```python
import functools

import jax
import jax.numpy as jnp
from jax import lax
from jax.experimental import pallas as pl
from jax.experimental.pallas import tpu as pltpu
from jax.sharding import PartitionSpec as P


HD = 128
F32 = jnp.float32
BF16 = jnp.bfloat16
MATMUL = (((1,), (0,)), ((), ()))
ROWS = (((0,), (0,)), ((), ()))
LANES = (((1,), (1,)), ((), ()))


def dot(a, b, dims=MATMUL):
    return lax.dot_general(a, b, dims, preferred_element_type=F32)


def kernel_call(body, ins, outs, scratch=(), flops=1_000_000_000, **static):
    place = {"s": pltpu.SMEM, "v": pltpu.VMEM, "h": pltpu.HBM}

    def call(*operands):
        letters = ins + ins[-1] * (len(operands) - len(ins))
        operands = [
            pltpu.with_memory_space_constraint(y, pltpu.HBM) if x == "h" else y
            for x, y in zip(letters, operands)
        ]
        return pl.pallas_call(
            functools.partial(body, **static),
            in_specs=[pl.BlockSpec(memory_space=place[x]) for x in letters],
            out_specs=[pl.BlockSpec(memory_space=place[x]) for x, _, _ in outs],
            out_shape=[
                (pltpu.HBM if x == "h" else jax.ShapeDtypeStruct)(shape, kind)
                for x, shape, kind in outs
            ],
            scratch_shapes=list(scratch),
            cost_estimate=pl.CostEstimate(flops=flops, bytes_accessed=4_000_000, transcendentals=0),
            compiler_params=pltpu.CompilerParams(vmem_limit_bytes=24 * 1024 * 1024),
        )(*operands)

    return call


def block_at(i, d, n):
    if n != 4 or d in (0, 3):
        return i ^ d
    inside = ((i >> 1) ^ i) & 1
    return i ^ (1 + inside if d == 1 else 2 - inside)


class Copies:
    def __init__(self, sems):
        self.sems, self.n = sems, 0

    def start(self, source, target):
        copy = pltpu.make_async_copy(source, target, self.sems.at[self.n])
        self.n += 1
        copy.start()
        return copy


def route_kernel(
    i_ref, me_ref, ids_ref, cot_hbm, put_ref, slot_ref, *refs, groups, slots
):
    sends, (cot_ref, buf, sems) = refs[:-3], refs[-3:]
    tokens, rows_n = put_ref.shape
    width = cot_ref.shape[1]
    part = width // groups
    copies = Copies(sems)
    loads = []
    for d in range(groups):
        source = pl.multiple_of(block_at(i_ref[0], d, groups) * part, HD)
        loads.append(
            copies.start(
                cot_hbm.at[0, :, pl.ds(source, part)], cot_ref.at[:, pl.ds(d * part, part)]
            )
        )
    id_0, id_1 = ids_ref[0, :, 0:1], ids_ref[0, :, 1:2]
    lanes = lax.broadcasted_iota(jnp.int32, (tokens, HD), 1)
    hit_0, hit_1 = lanes == id_0, lanes == id_1
    count = jnp.where(hit_0, 1.0, jnp.where(hit_1, 1.0, 0.0)).astype(BF16)
    row = lax.broadcasted_iota(jnp.int32, (tokens, tokens), 0)
    col = lax.broadcasted_iota(jnp.int32, (tokens, tokens), 1)
    before = dot(jnp.where(row > col, 1.0, 0.0).astype(BF16), count)
    rank_0 = jnp.sum(jnp.where(hit_0, before, 0.0), axis=1, keepdims=True).astype(jnp.int32)
    rank_1 = jnp.sum(jnp.where(hit_1, before, 0.0), axis=1, keepdims=True).astype(jnp.int32)
    slot_0, slot_1 = id_0 * slots + rank_0, id_1 * slots + rank_1
    slot_ref[:, 0:1] = slot_0
    slot_ref[:, 1:2] = slot_1
    wide = lax.broadcasted_iota(jnp.int32, (tokens, rows_n), 1)
    put = jnp.where(wide == slot_0, 1.0, jnp.where(wide == slot_1, 1.0, 0.0)).astype(BF16)
    put_ref[...] = put
    both = jnp.broadcast_to((id_0 + id_1).astype(F32), (tokens, HD)).astype(BF16)
    buf[:, pl.ds(width, HD)] = dot(put, both, ROWS).astype(BF16)
    for d in range(groups):
        at = pl.ds(d * part, part)
        loads[d].wait()
        buf[:, at] = dot(put, cot_ref[:, at], ROWS).astype(BF16)
    if len(sends) == 1:
        stores = [copies.start(buf, sends[0])]
    else:
        stores = [
            copies.start(buf.at[pl.ds(pl.multiple_of((me_ref[0] ^ k) * slots, 16), slots)], send)
            for k, send in enumerate(sends)
        ]
    for copy in stores:
        copy.wait()


def load_rows(copies, me, pieces, target, slots):
    if len(pieces) == 1:
        return [copies.start(pieces[0], target)]
    return [
        copies.start(piece, target.at[pl.ds(pl.multiple_of((me ^ k) * slots, 16), slots)])
        for k, piece in enumerate(pieces)
    ]


def state_kernel(k_hbm, v_hbm, out_ref, k_ref, v_ref, sems, *, heads, chunks):
    copies = Copies(sems)
    size = heads // chunks
    loads = []
    for c in range(chunks):
        at = pl.ds(c * size * HD, size * HD)
        loads.append(
            [
                copies.start(k_hbm.at[0, :, at], k_ref.at[:, at]),
                copies.start(v_hbm.at[0, :, at], v_ref.at[:, at]),
            ]
        )
    for h in range(heads):
        if h % size == 0:
            for copy in loads[h // size]:
                copy.wait()
        at = pl.ds(h * HD, HD)
        out_ref[h] = dot(k_ref[:, at], v_ref[:, at], ROWS).astype(BF16)


def intra_kernel(q_ref, k_ref, v_ref, out_ref, *, heads):
    tokens = q_ref.shape[1]
    row = lax.broadcasted_iota(jnp.int32, (tokens, tokens), 0)
    col = lax.broadcasted_iota(jnp.int32, (tokens, tokens), 1)
    causal = row >= col
    for h in range(heads):
        at = pl.ds(h * HD, HD)
        scores = dot(q_ref[0, :, at], k_ref[0, :, at], LANES)
        scores = jnp.where(causal, scores, 0.0).astype(BF16)
        out_ref[:, at] = dot(scores, v_ref[0, :, at])


def norm_kernel(
    i_ref, q_ref, prefix_ref, intra_ref, residual_ref, attn_ref, moe_ref, put_ref,
    stream_out, normed_out, send_out, stream_ref, normed_ref, send_ref, sems, *, heads, groups,
):
    tokens, width = stream_ref.shape
    copies, started = Copies(sems), []
    squares = jnp.zeros((tokens, HD), F32)
    for h in range(heads):
        at = pl.ds(h * HD, HD)
        attended = intra_ref[:, at] + dot(q_ref[0, :, at], prefix_ref[h])
        mean = jnp.mean(attended * attended, axis=-1, keepdims=True)
        attended = attended * lax.rsqrt(mean + 1e-06)
        stream = residual_ref[0, :, at].astype(F32) + attended * attn_ref[:, at]
        stream_ref[:, at] = stream
        squares = squares + stream * stream
    started.append(copies.start(stream_ref, stream_out))
    scale = lax.rsqrt(jnp.sum(squares, axis=-1, keepdims=True) / width + 1e-06)
    part = width // groups
    for h in range(heads):
        at = pl.ds(h * HD, HD)
        normed_ref[:, at] = (stream_ref[:, at] * scale * moe_ref[:, at]).astype(BF16)
    put = put_ref[...]
    started.append(copies.start(normed_ref, normed_out))
    for d in range(groups):
        at = pl.ds(d * part, part)
        source = pl.multiple_of(block_at(i_ref[0], d, groups) * part, HD)
        send_ref[:, at] = dot(put, normed_ref[:, pl.ds(source, part)], ROWS).astype(BF16)
        started.append(copies.start(send_ref.at[:, at], send_out.at[:, at]))
    for copy in started:
        copy.wait()


def load_weights(copies, own, got, groups, target, cuts):
    loads = [[copies.start(x.at[0], target.at[0, :, c]) for x, c in zip(own, cuts[0])]]
    for d in range(1, groups):
        loads.append([copies.start(got[d - 1].at[:, cuts[1]], target.at[d])])
    return loads


def cot_kernel(me_ref, down_hbm, *refs, groups, pieces, slots):
    got, cots = refs[: groups - 1], refs[groups - 1 : groups - 1 + pieces]
    out_ref, tag_hbm, cot_ref, tag_ref, w_ref, sems = refs[groups - 1 + pieces :]
    part, ff = w_ref.shape[1:]
    copies = Copies(sems)
    cot_loads = load_rows(copies, me_ref[0], cots, cot_ref, slots)
    cuts = ([pl.ds(0, ff)], pl.ds(2 * ff, ff))
    loads = load_weights(copies, [down_hbm], got, groups, w_ref, cuts)
    for copy in cot_loads:
        copy.wait()
    tag_ref[...] = cot_ref[:, pl.ds(cot_ref.shape[1] - HD, HD)].astype(F32)
    store = copies.start(tag_ref, tag_hbm)
    for copy in [x for load in loads for x in load]:
        copy.wait()
    total = dot(cot_ref[:, :part], w_ref[0])
    for d in range(1, groups):
        total = total + dot(cot_ref[:, pl.ds(d * part, part)], w_ref[d])
    out_ref[...] = total
    store.wait()


def rows_kernel(me_ref, rows_ref, router_hbm, tag_hbm, gate_hbm, up_hbm, *refs, groups):
    got = refs[: groups - 1]
    out_ref, share_ref, router_ref, tag_ref, w_ref, sems = refs[groups - 1 :]
    part = w_ref.shape[1]
    ff = w_ref.shape[2] // 2
    copies = Copies(sems)
    router_load = copies.start(router_hbm, router_ref)
    cuts = ([pl.ds(0, ff), pl.ds(ff, ff)], pl.ds(0, 2 * ff))
    loads = load_weights(copies, [gate_hbm, up_hbm], got, groups, w_ref, cuts)
    tag_load = copies.start(tag_hbm, tag_ref)
    router_load.wait()
    logits = dot(rows_ref[...], router_ref[...], LANES)
    total = None
    for d in range(groups):
        for copy in loads[d]:
            copy.wait()
        value = dot(rows_ref[:, pl.ds(d * part, part)], w_ref[d])
        total = value if total is None else total + value
    out_ref[...] = total
    tag_load.wait()
    lanes = lax.broadcasted_iota(jnp.int32, logits.shape, 1)
    me = me_ref[0]
    other = tag_ref[...].astype(jnp.int32)[:, : logits.shape[1]] - me
    sig = 1.0 / (1.0 + jnp.exp(-logits))
    own_sig = jnp.sum(jnp.where(lanes == me, sig, 0.0), axis=1, keepdims=True)
    other_sig = jnp.sum(jnp.where(lanes == other, sig, 0.0), axis=1, keepdims=True)
    share_ref[...] = jnp.broadcast_to(own_sig / (own_sig + other_sig), share_ref.shape)


def expert_kernel(
    me_ref, pre_ref, back_ref, share_ref, rows_ref, *refs, groups, last, pieces, slots
):
    got, cots = refs[:last], refs[last : last + pieces]
    hidden_ref, gated_ref, delta_ref, inner_ref, down_ref = refs[last + pieces : -2]
    cot_ref, sems = refs[-2:]
    part = cot_ref.shape[1]
    ff = hidden_ref.shape[1]
    copies = Copies(sems)
    at = pl.ds((groups - 1) * part, part)
    cot_loads = load_rows(copies, me_ref[0], [x.at[:, at] for x in cots], cot_ref, slots)
    mats = got[0][...] if last == 1 else got[0][...] + got[1][...]
    pre_gate = pre_ref[:, :ff] + dot(rows_ref[:, at], mats[:, :ff])
    pre_up = pre_ref[:, ff:] + dot(rows_ref[:, at], mats[:, ff : 2 * ff])
    gate = share_ref[:, 0:1]
    sigma = 1.0 / (1.0 + jnp.exp(-pre_gate))
    act = pre_gate * sigma
    hidden = act * pre_up
    hidden_ref[...] = hidden.astype(BF16)
    gated_ref[...] = (hidden * gate).astype(BF16)
    for copy in cot_loads:
        copy.wait()
    down_ref[...] = dot(cot_ref[...], gated_ref[...], ROWS).astype(BF16)
    d_hidden = (back_ref[...] + dot(cot_ref[...], mats[:, 2 * ff :])) * gate
    delta_ref[:, :ff] = (d_hidden * pre_up * sigma * (1.0 + pre_gate * (1.0 - sigma))).astype(BF16)
    delta_ref[:, ff:] = (d_hidden * act).astype(BF16)
    inner_ref[...] = dot(rows_ref[:, at], delta_ref[...], ROWS).astype(BF16)


def output_kernel(
    me_ref, hidden_ref, gated_ref, delta_ref, rows_ref, *refs, groups, last, pieces, slots
):
    late, refs = refs[:last], refs[last:]
    own, early, cots = refs[0], refs[1 : groups - 1], refs[groups - 1 : groups - 1 + pieces]
    out_hbm, *terms = refs[groups - 1 + pieces : -4]
    cot_ref, w_ref, out_ref, sems = refs[-4:]
    width = rows_ref.shape[1]
    part = width // groups
    ff = hidden_ref.shape[1]
    copies = Copies(sems)
    cot_loads = load_rows(copies, me_ref[0], cots, cot_ref, slots)
    cuts = ([pl.ds(0, ff)], pl.ds(2 * ff, ff))
    loads = load_weights(copies, [own], early, groups - 1, w_ref, cuts)
    for d in range(groups - 1):
        at = pl.ds(d * part, part)
        terms[2 * d + 1][...] = dot(rows_ref[:, at], delta_ref[...], ROWS).astype(BF16)
    for copy in cot_loads:
        copy.wait()
    for d in range(groups - 1):
        at = pl.ds(d * part, part)
        terms[2 * d][...] = dot(cot_ref[:, at], gated_ref[...], ROWS).astype(BF16)
    stores = []
    for d in range(groups):
        if d < groups - 1:
            for copy in loads[d]:
                copy.wait()
            mats = w_ref[d]
        else:
            mats = late[0][:, 2 * ff :]
            if last == 2:
                mats = mats + late[1][:, 2 * ff :]
        at = pl.ds(d * part, part)
        out_ref[:, at] = dot(hidden_ref[...], mats, LANES).astype(BF16)
        stores.append(copies.start(out_ref.at[:, at], out_hbm.at[:, at]))
    for copy in stores:
        copy.wait()


def combine_kernel(
    i_ref, stream_ref, normed_ref, router_ref, ids_ref, slot_ref, back_ref, out_ref, *, groups
):
    tokens, width = stream_ref.shape
    rows_n = back_ref.shape[0]
    logits = dot(normed_ref[...], router_ref[...], LANES)
    sig = 1.0 / (1.0 + jnp.exp(-logits))
    lanes = lax.broadcasted_iota(jnp.int32, logits.shape, 1)
    sig_0, sig_1 = (
        jnp.sum(jnp.where(lanes == ids_ref[0, :, j : j + 1], sig, 0.0), axis=1, keepdims=True)
        for j in range(2)
    )
    total = sig_0 + sig_1
    wide = lax.broadcasted_iota(jnp.int32, (tokens, rows_n), 1)
    take = jnp.where(
        wide == slot_ref[:, 0:1],
        sig_0 / total,
        jnp.where(wide == slot_ref[:, 1:2], sig_1 / total, 0.0),
    ).astype(BF16)
    part = width // groups
    for d in range(groups):
        at = pl.ds(pl.multiple_of(block_at(i_ref[0], d, groups) * part, HD), part)
        value = stream_ref[:, at] + dot(take, back_ref[:, pl.ds(d * part, part)])
        out_ref[0, :, at] = value.astype(BF16)


def total_kernel(scale_ref, *refs, outputs, parts_n, chunks):
    parts, outs = refs[:parts_n], refs[parts_n : parts_n + outputs]
    part_ref, out_ref, sems = refs[parts_n + outputs :]
    copies = Copies(sems)
    rows_n = out_ref.shape[0]
    size = rows_n // chunks
    ff = outs[0].shape[1]
    scale = jnp.where(scale_ref[0] > 0, 1.0, 0.0)
    loads, stores = [], []
    for c in range(chunks):
        at = pl.ds(c * size, size)
        loads.append([copies.start(x.at[at], part_ref.at[n, at]) for n, x in enumerate(parts)])
    for c in range(chunks):
        at = pl.ds(c * size, size)
        for copy in loads[c]:
            copy.wait()
        value = part_ref[0, at].astype(F32)
        for n in range(1, parts_n):
            value = value + part_ref[n, at].astype(F32)
        out_ref[at] = value * scale
        for n, out in enumerate(outs):
            stores.append(copies.start(out_ref.at[at, pl.ds(n * ff, ff)], out.at[at]))
    for copy in stores:
        copy.wait()


def total_call(trainable, parts, outputs):
    rows_n, columns = parts[0].shape
    chunks = 4
    return kernel_call(
        total_kernel,
        "sh",
        [("h", (rows_n, columns // outputs), F32)] * outputs,
        [
            pltpu.VMEM((len(parts), rows_n, columns), BF16),
            pltpu.VMEM((rows_n, columns), F32),
            pltpu.SemaphoreType.DMA((chunks * (len(parts) + outputs),)),
        ],
        outputs=outputs,
        parts_n=len(parts),
        chunks=chunks,
    )(trainable, *parts)


def exclusive_prefix(local, axis):
    n, i = lax.axis_size(axis), lax.axis_index(axis)
    half = local.shape[0] // 2
    core = i % 2
    mine = lax.dynamic_slice_in_dim(local, core * half, half, 0)
    other = lax.dynamic_slice_in_dim(local, (1 - core) * half, half, 0)
    swap = [(j, j ^ 1) for j in range(n)]
    peer = lax.ppermute(other, axis, swap).astype(F32)
    mine = mine.astype(F32)
    total = mine + peer
    before = jnp.zeros_like(mine)
    step = 2
    while step < n:
        last = 2 * step >= n
        pairs = [(j, j ^ step) for j in range(n) if not (last and j & step)]
        got = lax.ppermute(total.astype(BF16), axis, pairs).astype(F32)
        before = before + jnp.where((i & step) != 0, got, 0.0)
        total = total + got
        step *= 2
    own = before + jnp.where(core == 1, peer, 0.0)
    theirs = before + jnp.where(core == 0, mine, 0.0)
    back = lax.ppermute(theirs.astype(BF16), axis, swap)
    own = own.astype(BF16)
    return jnp.where(core == 0, jnp.concatenate([own, back], 0), jnp.concatenate([back, own], 0))


def send_xor(x, axis, d):
    return lax.ppermute(x, axis, [(j, j ^ d) for j in range(lax.axis_size(axis))])


ENDS = [(0, 1), (3, 2)]
MIDDLE = [(1, 2), (2, 1)]
FIRST = [(0, 2), (3, 1), (1, 0), (2, 3)]
SECOND = [(1, 3), (2, 0), (0, 1), (3, 2)]


def gather_line(x, axis):
    n = lax.axis_size(axis)
    if n != 4:
        return [send_xor(x, axis, d) for d in range(1, n)]
    first = lax.ppermute(x, axis, FIRST)
    second = lax.ppermute(x, axis, SECOND)
    relayed = lax.ppermute(first, axis, [(b, a) for a, b in ENDS])
    middle = lax.ppermute(x, axis, MIDDLE)
    return [first, second, relayed, middle]


def scatter_line(parts, axis):
    n = lax.axis_size(axis)
    if n != 4:
        return [parts[0]] + [send_xor(parts[d], axis, d) for d in range(1, n)]
    relayed = lax.ppermute(parts[3], axis, ENDS)
    middle = lax.ppermute(parts[3], axis, MIDDLE)
    second = lax.ppermute(parts[2], axis, [(b, a) for a, b in SECOND])
    merged = (parts[1].astype(F32) + relayed.astype(F32)).astype(BF16)
    first = lax.ppermute(merged, axis, [(b, a) for a, b in FIRST])
    return [parts[0], middle, second, first]


def exchange(x):
    return lax.all_to_all(x, "seq", split_axis=0, concat_axis=0, tiled=True)


def exchange_pieces(blocks):
    n = len(blocks)
    got = [blocks[0]]
    for k in range(1, n):
        got.append(send_xor(blocks[k], "seq", k))
    return got


def swap_blocks(x, axis, dim):
    n, i = lax.axis_size(axis), lax.axis_index(axis)
    size = x.shape[dim] // n
    return jnp.concatenate(
        [lax.dynamic_slice_in_dim(x, block_at(i, d, n) * size, size, dim) for d in range(n)], axis=dim
    )


def layer(
    queries,
    keys,
    values,
    residual_in,
    cotangent,
    expert_ids,
    router,
    attn_gain,
    moe_gain,
    w_gate,
    w_up,
    w_down,
    trainable,
):
    tokens = queries.shape[1]
    width = queries.shape[2]
    heads = width // HD
    experts = router.shape[1]
    peers = lax.axis_size("seq")
    groups = lax.axis_size("dp")
    slots = max(2, 3 * tokens // peers)
    rows_n = experts * slots
    part = width // groups
    ff = w_gate.shape[2]
    i = lax.axis_index("dp")[None]
    me = lax.axis_index("seq")[None]
    turned = swap_blocks(router.T, "dp", 1)

    split = slots % 16 == 0
    cot_shape = (slots if split else rows_n, width + HD)
    pieces = peers if split else 1
    put, slot, *cot_send = kernel_call(
        route_kernel,
        "ssvh",
        [("v", (tokens, rows_n), BF16), ("v", (tokens, 2), jnp.int32)]
        + [("h", cot_shape, BF16)] * pieces,
        [
            pltpu.VMEM((tokens, width), BF16),
            pltpu.VMEM((rows_n, width + HD), BF16),
            pltpu.SemaphoreType.DMA((groups + pieces,)),
        ],
        groups=groups,
        slots=slots,
    )(i, me, expert_ids, cotangent)
    if split:
        cots = exchange_pieces(cot_send)
    else:
        cots = [exchange(cot_send[0].reshape(experts, slots, -1)).reshape(cot_shape)]

    got = gather_line(jnp.concatenate([w_gate[0], w_up[0], w_down[0]], axis=1), "dp")

    (local,) = kernel_call(
        state_kernel,
        "h",
        [("v", (heads, HD, HD), BF16)],
        [
            pltpu.VMEM((tokens, width), BF16),
            pltpu.VMEM((tokens, width), BF16),
            pltpu.SemaphoreType.DMA((8,)),
        ],
        heads=heads,
        chunks=4,
    )(keys, values)
    prefix = exclusive_prefix(local, "seq")

    (intra,) = kernel_call(
        intra_kernel, "v", [("v", (tokens, width), F32)], heads=heads
    )(queries, keys, values)
    stream, normed, send_rows = kernel_call(
        norm_kernel,
        "sv",
        [
            ("h", (tokens, width), F32),
            ("h", (tokens, width), BF16),
            ("h", (rows_n, width), BF16),
        ],
        [
            pltpu.VMEM((tokens, width), F32),
            pltpu.VMEM((tokens, width), BF16),
            pltpu.VMEM((rows_n, width), BF16),
            pltpu.SemaphoreType.DMA((groups + 2,)),
        ],
        heads=heads,
        groups=groups,
    )(i, queries, prefix, intra, residual_in, attn_gain[None], moe_gain[None], put)
    rows = exchange(send_rows.reshape(experts, slots, width)).reshape(rows_n, width)

    early = got[: groups - 2]
    late = got[groups - 2 :]
    cot_part, tags = kernel_call(
        cot_kernel,
        "sh",
        [("v", (rows_n, ff), F32), ("h", (rows_n, HD), F32)],
        [
            pltpu.VMEM((rows_n, width + HD), BF16),
            pltpu.VMEM((rows_n, HD), F32),
            pltpu.VMEM((groups - 1, part, ff), BF16),
            pltpu.SemaphoreType.DMA((groups + 1 + pieces,)),
        ],
        groups=groups - 1,
        pieces=pieces,
        slots=slots,
    )(me, w_down, *early, *cots)
    row_part, share = kernel_call(
        rows_kernel,
        "svh",
        [("v", (rows_n, 2 * ff), F32), ("v", (rows_n, HD), F32)],
        [
            pltpu.VMEM((experts, width), BF16),
            pltpu.VMEM((rows_n, HD), F32),
            pltpu.VMEM((groups - 1, part, 2 * ff), BF16),
            pltpu.SemaphoreType.DMA((groups + 2,)),
        ],
        groups=groups - 1,
    )(me, rows, turned, tags, w_gate, w_up, *early)
    hidden, gated, delta, far_inner, far_down = kernel_call(
        expert_kernel,
        "svvvv" + "v" * len(late) + "h",
        [
            ("v", (rows_n, ff), BF16),
            ("v", (rows_n, ff), BF16),
            ("v", (rows_n, 2 * ff), BF16),
            ("v", (part, 2 * ff), BF16),
            ("v", (part, ff), BF16),
        ],
        [
            pltpu.VMEM((rows_n, part), BF16),
            pltpu.SemaphoreType.DMA((pieces,)),
        ],
        groups=groups,
        last=len(late),
        pieces=pieces,
        slots=slots,
    )(me, row_part, cot_part, share, rows, *late, *cots)
    expert_out, *terms = kernel_call(
        output_kernel,
        "svvvv" + "v" * len(late) + "h",
        [("h", (rows_n, width), BF16)]
        + [("v", (part, ff), BF16), ("v", (part, 2 * ff), BF16)] * (groups - 1),
        [
            pltpu.VMEM((rows_n, width + HD), BF16),
            pltpu.VMEM((groups - 1, part, ff), BF16),
            pltpu.VMEM((rows_n, width), BF16),
            pltpu.SemaphoreType.DMA((2 * groups + pieces,)),
        ],
        groups=groups,
        last=len(late),
        pieces=pieces,
        slots=slots,
    )(me, hidden, gated, delta, rows, *late, w_down, *early, *cots)
    down_parts = scatter_line(terms[0::2] + [far_down], "dp")
    inner_parts = scatter_line(terms[1::2] + [far_inner], "dp")
    back = exchange(expert_out.reshape(peers, slots, width)).reshape(rows_n, width)
    (mixed,) = kernel_call(
        combine_kernel, "sv", [("v", (1, tokens, width), BF16)], groups=groups
    )(i, stream, normed, router.T, expert_ids, slot, back)
    mixed, *inner_parts = lax.optimization_barrier((mixed, *inner_parts))
    (grad_down,) = total_call(trainable, down_parts, 1)
    grad_gate, grad_up = total_call(trainable, inner_parts, 2)
    return (mixed, grad_gate[None], grad_up[None], grad_down[None])


def solution(mesh):
    return jax.shard_map(
        layer,
        mesh=mesh,
        in_specs=(
            P("dp", "seq", None),
            P("dp", "seq", None),
            P("dp", "seq", None),
            P("dp", "seq", None),
            P("dp", "seq", None),
            P("dp", "seq", None),
            P(),
            P(),
            P(),
            P("seq", "dp", None),
            P("seq", "dp", None),
            P("seq", "dp", None),
            P("seq"),
        ),
        out_specs=(
            P("dp", "seq", None),
            P("seq", "dp", None),
            P("seq", "dp", None),
            P("seq", "dp", None),
        ),
        check_vma=False,
    )
```
